32 devices in a mesh: py: 4 (over y, core), px: 2 (over x), pz: 4 (over z).
Axes of the slice: x: 2, y: 2, z: 4, core: 2. Of those that a mesh axis runs over, the one named last changes fastest.
Arguments:
- starting_state: float32 [512, 8, 128, 128], P('py', 'px', 'pz'), may hold values from 0.5 to 2
- scaled_conductivity: float32 [512, 8, 128, 128], P('py', 'px', 'pz'), may hold values from 0.03 to 0.15
- scaled_heat_supply: float32 [512, 8, 128, 128], P('py', 'px', 'pz'), may hold values from -0.2 to 0.2
Outputs:
- normalised_result: float32 [512, 8, 128, 128], P('py', 'px', 'pz')
- temperature_end: float32 [512, 8, 128, 128], P('py', 'px', 'pz')
The draws below stay inside these ranges and needn't reach their ends.
All inputs are finite; a program needn't handle non-finite values.
Results may differ from the reference program's by a relative error of at most 0.00002.
Values sent between devices are 32-bit elements; how exact they have to be, the bound alone decides.
A program may use at most 128 MiB of HBM per device.

```python
import jax
import jax.numpy as jnp
from jax import lax

GRID_DEPTH = 512
GRID_WIDTH = 8
GRID_HEIGHT = 128
SAMPLE_TOTAL = 128
STEPS = 4


def block_levels(rng, shape, split, low, high):
    def one(position, parts):
        heights = jax.random.uniform(jax.random.fold_in(jax.random.fold_in(rng, 6), position), (parts,), jnp.float32, low / len(split), high / len(split))
        return jnp.repeat(jnp.exp(heights), shape[position] // parts).reshape((-1,) + (1,) * (len(shape) - position - 1))

    level = one(*split[0])
    for cut in split[1:]:
        level = level * one(*cut)
    return level


def setup_inputs(seed: int = 0) -> dict:
    keys = jax.random.split(jax.random.key(seed), 4)
    return {
        "starting_state": jnp.clip(0.5 + 1.5 * jax.random.uniform(keys[0], (GRID_DEPTH, GRID_WIDTH, GRID_HEIGHT, SAMPLE_TOTAL), jnp.float32) ** block_levels(keys[0], (GRID_DEPTH, GRID_WIDTH, GRID_HEIGHT, SAMPLE_TOTAL), ((0, 4), (1, 2), (2, 4)), -0.2, 0.2), 0.5, 2.0),
        "scaled_conductivity": jnp.clip(0.03 + 0.120000007 * jax.random.uniform(keys[1], (GRID_DEPTH, GRID_WIDTH, GRID_HEIGHT, SAMPLE_TOTAL), jnp.float32) ** block_levels(keys[1], (GRID_DEPTH, GRID_WIDTH, GRID_HEIGHT, SAMPLE_TOTAL), ((0, 4), (1, 2), (2, 4)), -0.2, 0.2), 0.03, 0.15),
        "scaled_heat_supply": jnp.clip(jax.random.uniform(keys[2], (GRID_DEPTH, GRID_WIDTH, GRID_HEIGHT, SAMPLE_TOTAL), jnp.float32, -0.2, 0.2) * block_levels(keys[2], (GRID_DEPTH, GRID_WIDTH, GRID_HEIGHT, SAMPLE_TOTAL), ((0, 4), (1, 2), (2, 4)), -0.4, 0.0), -0.2, 0.2),
    }


def interior_points(values, dims):
    for coordinate_axis in dims:
        values = lax.slice_in_dim(values, 1, values.shape[coordinate_axis] - 1, axis=coordinate_axis)
    return values

def boundary_layer(values, coordinate_axis, start, dims):
    others = [other for other in dims if other != coordinate_axis]
    values = interior_points(values, others)
    return lax.slice_in_dim(values, start, start + values.shape[coordinate_axis] - 2, axis=coordinate_axis)

def conduction_timestep(framed_thermal_lattice, scaled_conductivity, scaled_heat_supply):
    central_point = interior_points(framed_thermal_lattice, (0, 1, 2))
    preceding_neighbour = [boundary_layer(framed_thermal_lattice, coordinate_axis, 0, (0, 1, 2)) for coordinate_axis in (0, 1, 2)]
    following_neighbour = [boundary_layer(framed_thermal_lattice, coordinate_axis, 2, (0, 1, 2)) for coordinate_axis in (0, 1, 2)]
    spread = preceding_neighbour[0] + following_neighbour[0] + preceding_neighbour[1] + following_neighbour[1] + preceding_neighbour[2] + following_neighbour[2] - 6.0 * central_point
    return central_point + scaled_conductivity * spread + scaled_heat_supply

def reference(starting_state, scaled_conductivity, scaled_heat_supply):
    for step in range(STEPS):
        starting_state = conduction_timestep(jnp.pad(starting_state, ((1, 1), (1, 1), (1, 1), (0, 0)), mode='constant'), scaled_conductivity, scaled_heat_supply)
    row_average = lax.optimization_barrier(jnp.mean(starting_state, axis=1, keepdims=True))
    deviation_rows = starting_state - row_average
    line_variance = lax.optimization_barrier(jnp.mean(deviation_rows * deviation_rows, axis=1, keepdims=True))
    normalised_result = deviation_rows * lax.rsqrt(line_variance + 0.0001)
    return (normalised_result, starting_state)
```

```python
import functools

import jax
import jax.numpy as jnp
from jax import lax
from jax.experimental import pallas as pl
from jax.experimental.pallas import tpu as pltpu
from jax.sharding import PartitionSpec as P

STEPS = 4
MESH = pl.DeviceIdType.MESH


def left_over(rows, pieces, turn):
    size = rows // pieces
    return (size, size) if turn == 0 else (max(size // 4, 1), 0)


def cut_pieces(rows, pieces):
    size = rows // pieces
    cut = set()
    for turn in (0, 1):
        head, foot = left_over(rows, pieces, turn)
        cut |= {k for k in range(pieces) if k * size < head or (k + 1) * size > rows - foot}
    return sorted(cut)


def normalise(mine, sums, others):
    width = mine.shape[0]
    gap = sums[0] - others[0]
    mean = 0.5 * (sums[0] + others[0])
    variance = (sums[1] + others[1]) * (0.5 / width) + 0.25 * gap * gap
    return (mine - mean[None]) * lax.rsqrt(variance + 0.0001)[None]


def kernel(pieces, pair, *refs):
    if pair:
        (u_in, c_in, s_in, c, s, sq, u, zh, sqr,
         load, xs, xr, ys, yr, zs, zr, qs, qr) = refs
    else:
        (u_in, c_in, s_in, s, u, zh, c,
         load, xs, xr, ys, yr, zs, zr) = refs
    rows, width, height, lanes = c.shape
    size = rows // pieces
    half = pieces // 2

    names = ("py", "px", "pz")
    here = {name: lax.axis_index(name) for name in names}
    last = {name: lax.axis_size(name) - 1 for name in names}

    def has(name, side):
        return here[name] > 0 if side == 0 else here[name] < last[name]

    def beside(name, side):
        return {name: here[name] + (2 * side - 1)}

    def piece(p):
        odd = p % 2
        return half + (p // 2) * (1 - 2 * odd) - odd

    def span(k, pad=0):
        return pl.ds(k * size + pad, size)

    inner = pl.ds(1, width)

    def load_copy(which, k):
        if which == 0:
            return pltpu.make_async_copy(
                u_in.at[span(k)], u.at[0, span(k, 1), inner], load.at[0, k])
        src, dst = ((c_in, c), (s_in, s))[which - 1]
        return pltpu.make_async_copy(src.at[span(k)], dst.at[span(k)], load.at[which, k])

    def x_copy(slot, side, k, to):
        return pltpu.make_async_remote_copy(
            src_ref=u.at[slot, span(k, 1), pl.ds(width if side else 1, 1)],
            dst_ref=u.at[slot, span(k, 1), pl.ds(0 if side else width + 1, 1)],
            send_sem=xs.at[slot, side, k], recv_sem=xr.at[slot, 1 - side, k],
            device_id=beside("px", to), device_id_type=MESH)

    def z_copy(slot, side, k, to):
        return pltpu.make_async_remote_copy(
            src_ref=u.at[slot, span(k, 1), inner, pl.ds(height - 1 if side else 0, 1)],
            dst_ref=zh.at[slot, 1 - side, span(k)],
            send_sem=zs.at[slot, side, k], recv_sem=zr.at[slot, 1 - side, k],
            device_id=beside("pz", to), device_id_type=MESH)

    def y_copy(slot, side, to):
        return pltpu.make_async_remote_copy(
            src_ref=u.at[slot, pl.ds(rows if side else 1, 1), inner],
            dst_ref=u.at[slot, pl.ds(0 if side else rows + 1, 1), inner],
            send_sem=ys.at[slot, side], recv_sem=yr.at[slot, 1 - side],
            device_id=beside("py", to), device_id_type=MESH)

    def each_side(slot, k, act):
        for side in (0, 1):
            @pl.when(has("px", side))
            def _(side=side):
                act(lambda d, t: x_copy(slot, d, k, t), side)

            @pl.when(has("pz", side))
            def _(side=side):
                act(lambda d, t: z_copy(slot, d, k, t), side)

            edge = pieces - 1 if side else 0

            @pl.when(jnp.logical_and(has("py", side), k == edge))
            def _(side=side):
                act(lambda d, t: y_copy(slot, d, t), side)

    def send(slot, k):
        each_side(slot, k, lambda copy, side: copy(side, side).start())

    def sent(slot, k):
        each_side(slot, k, lambda copy, side: copy(side, side).wait_send())

    def arrived(slot, k):
        each_side(slot, k, lambda copy, side: copy(1 - side, side).wait_recv())

    def sums_copy(k, rows_of):
        return pltpu.make_async_remote_copy(
            src_ref=sq.at[rows_of], dst_ref=sqr.at[rows_of],
            send_sem=qs.at[k], recv_sem=qr.at[k],
            device_id={"px": 1 - here["px"]}, device_id_type=MESH)

    def each_sum(k, act):
        cut = jnp.bool_(False)
        for e in cut_pieces(rows, pieces):
            cut = jnp.logical_or(cut, k == e)

        @pl.when(jnp.logical_not(cut))
        def _():
            act(sums_copy(k, span(k)), k * size, size)

        for turn in (0, 1):
            head, foot = left_over(rows, pieces, turn)
            for e in cut_pieces(rows, pieces):
                low, high = max(e * size, head), min((e + 1) * size, rows - foot)
                if high > low:
                    @pl.when(jnp.logical_and(k == e, here["py"] % 2 == turn))
                    def _(e=e, low=low, high=high):
                        act(sums_copy(e, pl.ds(low, high - low)), low, high - low)

    def over_pieces(act):
        def one(p, carry):
            act(piece(p))
            return carry
        lax.fori_loop(0, pieces, one, 0)

    barrier = pltpu.get_barrier_semaphore()
    count = 0
    for name in names:
        for side in (0, 1):
            there = has(name, side)
            count = count + there.astype(jnp.int32)

            @pl.when(there)
            def _(name=name, side=side):
                pl.semaphore_signal(
                    barrier, inc=1, device_id=beside(name, side), device_id_type=MESH)

    over_pieces(lambda k: load_copy(0, k).start())

    def load_rest(k):
        load_copy(1, k).start()
        load_copy(2, k).start()

    over_pieces(load_rest)

    pl.semaphore_wait(barrier, count)

    def first_send(k):
        load_copy(0, k).wait()
        send(0, k)

    over_pieces(first_send)

    for side in (0, 1):
        for slot in (0, 1):
            @pl.when(jnp.logical_not(has("py", side)))
            def _(side=side, slot=slot):
                u[slot, rows + 1 if side else 0, 1:width + 1] = jnp.zeros(
                    (width, height, lanes), jnp.float32)

            @pl.when(jnp.logical_not(has("px", side)))
            def _(side=side, slot=slot):
                def clear(r, carry):
                    u[slot, r + 1, width + 1 if side else 0] = jnp.zeros(
                        (height, lanes), jnp.float32)
                    return carry
                lax.fori_loop(0, rows, clear, 0)

            @pl.when(jnp.logical_not(has("pz", side)))
            def _(side=side, slot=slot):
                def clear(r, carry):
                    zh[slot, side, r] = jnp.zeros((width, 1, lanes), jnp.float32)
                    return carry
                lax.fori_loop(0, rows, clear, 0)

    level = lax.broadcasted_iota(jnp.int32, (width, height, lanes), 1)

    for step in range(1, STEPS + 1):
        old, new = (step - 1) % 2, step % 2

        def row(r, old, new, final):
            centre = u[old, r + 1, 1:width + 1]
            below = jnp.where(
                level == 0, zh[old, 0, r], pltpu.roll(centre, 1, axis=1))
            above = jnp.where(
                level == height - 1, zh[old, 1, r], pltpu.roll(centre, height - 1, axis=1))
            spread = (
                u[old, r, 1:width + 1]
                + u[old, r + 2, 1:width + 1]
                + u[old, r + 1, 0:width]
                + u[old, r + 1, 2:width + 2]
                + below
                + above
                - 6.0 * centre
            )
            value = centre + c[r] * spread + s[r]
            if final:
                s[r] = value
            else:
                u[new, r + 1, 1:width + 1] = value
            if final and pair:
                mean = jnp.sum(value, axis=0) * (1.0 / width)
                apart = value - mean[None]
                sq[r, 0] = mean
                sq[r, 1] = jnp.sum(apart * apart, axis=0)

        def sweep(k, step=step, old=old, new=new):
            if step == 1:
                load_copy(1, k).wait()
                load_copy(2, k).wait()
            arrived(old, k)
            if 2 <= step < STEPS:
                sent(new, k)

            def one(i, carry):
                row(k * size + i, old, new, step == STEPS)
                return carry
            lax.fori_loop(0, size, one, 0)
            if step < STEPS:
                send(new, k)
            elif pair:
                each_sum(k, lambda copy, first, count: copy.start())

        over_pieces(sweep)

    def finish(copy, first, count):
        copy.wait_recv()

        def one(i, carry):
            r = first + i
            c[r] = normalise(s[r], sq[r], sqr[r])
            return carry
        lax.fori_loop(0, count, one, 0)

    def close(k):
        for slot in sorted({(STEPS - 1) % 2, (STEPS - 2) % 2}):
            sent(slot, k)
        if pair:
            each_sum(k, lambda copy, first, count: copy.wait_send())

    if pair:
        over_pieces(lambda k: each_sum(k, finish))
    over_pieces(close)


def copy_all(copies):
    for copy in copies:
        copy.start()
    for copy in copies:
        copy.wait()


def put_out(pieces, count, *refs):
    held, out, done = refs[:count], refs[count:2 * count], refs[-1]
    size = held[0].shape[0] // pieces
    copy_all([
        pltpu.make_async_copy(
            held[i].at[pl.ds(k * size, size)], out[i].at[pl.ds(k * size, size)], done.at[i, k])
        for k in range(pieces)
        for i in range(count)
    ])


def put_most(pieces, result, end, result_out, end_out, mark, done):
    rows = end.shape[0]
    size = rows // pieces
    mark[...] = jnp.zeros(mark.shape, mark.dtype)
    for turn in (0, 1):
        @pl.when(lax.axis_index("py") % 2 == turn)
        def _(turn=turn):
            head, foot = left_over(rows, pieces, turn)
            copies = []
            for k in range(pieces):
                whole = pl.ds(k * size, size)
                copies.append(pltpu.make_async_copy(
                    end.at[whole], end_out.at[whole], done.at[0, k]))
                low, high = max(k * size, head), min((k + 1) * size, rows - foot)
                if high > low:
                    part = pl.ds(low, high - low)
                    copies.append(pltpu.make_async_copy(
                        result.at[part], result_out.at[part], done.at[1, k]))
            copy_all(copies)


def left_parts(rows, pieces, turn):
    size = rows // pieces
    head, foot = left_over(rows, pieces, turn)
    parts = [(rows - foot + i, head + i, min(size, foot - i)) for i in range(0, foot, size)]
    low = head
    while low > 0:
        count = min(size // 2, max(low // 2, size // 8, 1))
        low -= count
        parts.append((low, low, count))
    return parts


def exchange_rest(pieces, sums, end, mark, out, other, sent, got):
    rows = end.shape[0]
    partner = {"px": 1 - lax.axis_index("px")}
    barrier = pltpu.get_barrier_semaphore()
    pl.semaphore_signal(barrier, inc=1, device_id=partner, device_id_type=MESH)
    pl.semaphore_wait(barrier, 1)
    for turn in (0, 1):
        @pl.when(lax.axis_index("py") % 2 == turn)
        def _(turn=turn):
            parts = left_parts(rows, pieces, turn)
            copies = [
                pltpu.make_async_remote_copy(
                    src_ref=sums.at[pl.ds(row, count)], dst_ref=other.at[pl.ds(at, count)],
                    send_sem=sent.at[n], recv_sem=got.at[n],
                    device_id=partner, device_id_type=MESH)
                for n, (row, at, count) in enumerate(parts)
            ]
            for copy in copies:
                copy.start()
            for copy, (row, at, count) in zip(copies, parts):
                copy.wait_recv()

                def one(i, carry, row=row, at=at):
                    out[at + i] = normalise(end[row + i], sums[row + i], other[at + i])
                    return carry
                lax.fori_loop(0, count, one, 0)
            for copy in copies:
                copy.wait_send()


def put_rest(pieces, rest, result, result_out, done):
    rows = result.shape[0]
    for turn in (0, 1):
        @pl.when(lax.axis_index("py") % 2 == turn)
        def _(turn=turn):
            head, foot = left_over(rows, pieces, turn)
            pairs = [((rows - foot, head), foot), ((0, 0), head)]
            copy_all([
                pltpu.make_async_copy(
                    rest.at[pl.ds(at, count)], result_out.at[pl.ds(row, count)], done.at[n])
                for n, ((row, at), count) in enumerate(pairs) if count
            ])


def body(starting_state, scaled_conductivity, scaled_heat_supply):
    rows, width, height, lanes = starting_state.shape
    pieces = next(n for n in (8, 4, 2) if rows % n == 0)
    pair = lax.axis_size("px") == 2
    dma = pltpu.SemaphoreType.DMA
    block = jax.ShapeDtypeStruct(starting_state.shape, jnp.float32)
    field = pltpu.VMEM((rows, width, height, lanes), jnp.float32)
    sums = pltpu.VMEM((rows, 2, height, lanes), jnp.float32)
    here, there = pl.BlockSpec(memory_space=pltpu.VMEM), pl.BlockSpec(memory_space=pl.ANY)
    scratch = [
        pltpu.VMEM((2, rows + 2, width + 2, height, lanes), jnp.float32),
        pltpu.VMEM((2, 2, rows, width, 1, lanes), jnp.float32),
    ]
    scratch += [sums] if pair else [field]
    scratch += [
        dma((3, pieces)),
        dma((2, 2, pieces)), dma((2, 2, pieces)),
        dma((2, 2)), dma((2, 2)),
        dma((2, 2, pieces)), dma((2, 2, pieces)),
    ]
    scratch += [dma((pieces,)), dma((pieces,))] if pair else []
    made = (field, field, sums) if pair else (field,)
    outputs = pl.pallas_call(
        functools.partial(kernel, pieces, pair),
        out_shape=made,
        in_specs=[there] * 3,
        out_specs=(here,) * len(made),
        scratch_shapes=scratch,
        compiler_params=pltpu.CompilerParams(
            collective_id=0, has_side_effects=True, vmem_limit_bytes=(34 if pair else 40) * 1024 * 1024),
    )(starting_state, scaled_conductivity, scaled_heat_supply)
    if pair:
        held, end, kept = outputs
        result, end_out, mark = pl.pallas_call(
            functools.partial(put_most, pieces),
            out_shape=(block, block, pltpu.VMEM((8, 128), jnp.float32)),
            in_specs=[here] * 2,
            out_specs=(there, there, here),
            scratch_shapes=[dma((2, pieces))],
            compiler_params=pltpu.CompilerParams(vmem_limit_bytes=1024 * 1024),
        )(held, end)
        most = max(sum(left_over(rows, pieces, turn)) for turn in (0, 1))
        parts = max(len(left_parts(rows, pieces, turn)) for turn in (0, 1))
        rest = pl.pallas_call(
            functools.partial(exchange_rest, pieces),
            out_shape=pltpu.VMEM((most, width, height, lanes), jnp.float32),
            in_specs=[here] * 3,
            out_specs=here,
            scratch_shapes=[
                pltpu.VMEM((most, 2, height, lanes), jnp.float32), dma((parts,)), dma((parts,))],
            compiler_params=pltpu.CompilerParams(
                collective_id=1, has_side_effects=True, vmem_limit_bytes=4 * 1024 * 1024),
        )(kept, end, mark)
        result = pl.pallas_call(
            functools.partial(put_rest, pieces),
            out_shape=block,
            in_specs=[here, there],
            out_specs=there,
            scratch_shapes=[dma((2,))],
            input_output_aliases={1: 0},
            compiler_params=pltpu.CompilerParams(vmem_limit_bytes=1024 * 1024),
        )(rest, result)
        return result, end_out
    outputs = pl.pallas_call(
        functools.partial(put_out, pieces, len(outputs)),
        out_shape=(block,) * len(outputs),
        in_specs=[here] * len(outputs),
        out_specs=(there,) * len(outputs),
        scratch_shapes=[dma((len(outputs), pieces))],
        compiler_params=pltpu.CompilerParams(vmem_limit_bytes=1024 * 1024),
    )(*outputs)
    (end,) = outputs
    line = width * lax.axis_size("px")
    guess = 1.0
    moved = end - guess
    totals, squares = lax.psum(
        (jnp.sum(moved, axis=1, keepdims=True), jnp.sum(moved * moved, axis=1, keepdims=True)), "px"
    )
    row_average = guess + totals / line
    line_variance = squares / line - totals / line * (totals / line)
    return ((end - row_average) * lax.rsqrt(line_variance + 0.0001), end)


def solution(mesh):
    placed = P("py", "px", "pz", None)
    return jax.shard_map(
        body,
        mesh=mesh,
        in_specs=(placed, placed, placed),
        out_specs=(placed, placed),
        check_vma=False,
    )
```

```python
import functools

import jax
import jax.numpy as jnp
from jax import lax
from jax.experimental import pallas as pl
from jax.experimental.pallas import tpu as pltpu
from jax.sharding import PartitionSpec as P

STEPS = 4
MESH = pl.DeviceIdType.MESH


def left_over(rows, pieces, turn):
    size = rows // pieces
    return (size, size) if turn == 1 else (0, 0)


def cut_pieces(rows, pieces):
    size = rows // pieces
    cut = set()
    for turn in (0, 1):
        head, foot = left_over(rows, pieces, turn)
        cut |= {k for k in range(pieces) if k * size < head or (k + 1) * size > rows - foot}
    return sorted(cut)


def normalise(mine, sums, others):
    width = mine.shape[0]
    gap = sums[0] - others[0]
    mean = 0.5 * (sums[0] + others[0])
    variance = (sums[1] + others[1]) * (0.5 / width) + 0.25 * gap * gap
    return (mine - mean[None]) * lax.rsqrt(variance + 0.0001)[None]


def kernel(pieces, pair, *refs):
    if pair:
        (u_in, c_in, s_in, c, s, sq, u, zh, sqr,
         load, xs, xr, ys, yr, zs, zr, qs, qr) = refs
    else:
        (u_in, c_in, s_in, s, u, zh, c,
         load, xs, xr, ys, yr, zs, zr) = refs
    rows, width, height, lanes = c.shape
    size = rows // pieces
    half = pieces // 2

    names = ("py", "px", "pz")
    here = {name: lax.axis_index(name) for name in names}
    last = {name: lax.axis_size(name) - 1 for name in names}

    def has(name, side):
        return here[name] > 0 if side == 0 else here[name] < last[name]

    def beside(name, side):
        return {name: here[name] + (2 * side - 1)}

    def piece(p):
        odd = p % 2
        return half + (p // 2) * (1 - 2 * odd) - odd

    def span(k, pad=0):
        return pl.ds(k * size + pad, size)

    inner = pl.ds(1, width)

    def load_copy(which, k):
        if which == 0:
            return pltpu.make_async_copy(
                u_in.at[span(k)], u.at[0, span(k, 1), inner], load.at[0, k])
        src, dst = ((c_in, c), (s_in, s))[which - 1]
        return pltpu.make_async_copy(src.at[span(k)], dst.at[span(k)], load.at[which, k])

    def x_copy(slot, side, k, to):
        return pltpu.make_async_remote_copy(
            src_ref=u.at[slot, span(k, 1), pl.ds(width if side else 1, 1)],
            dst_ref=u.at[slot, span(k, 1), pl.ds(0 if side else width + 1, 1)],
            send_sem=xs.at[slot, side, k], recv_sem=xr.at[slot, 1 - side, k],
            device_id=beside("px", to), device_id_type=MESH)

    def z_copy(slot, side, k, to):
        return pltpu.make_async_remote_copy(
            src_ref=u.at[slot, span(k, 1), inner, pl.ds(height - 1 if side else 0, 1)],
            dst_ref=zh.at[slot, 1 - side, span(k)],
            send_sem=zs.at[slot, side, k], recv_sem=zr.at[slot, 1 - side, k],
            device_id=beside("pz", to), device_id_type=MESH)

    def y_copy(slot, side, to):
        return pltpu.make_async_remote_copy(
            src_ref=u.at[slot, pl.ds(rows if side else 1, 1), inner],
            dst_ref=u.at[slot, pl.ds(0 if side else rows + 1, 1), inner],
            send_sem=ys.at[slot, side], recv_sem=yr.at[slot, 1 - side],
            device_id=beside("py", to), device_id_type=MESH)

    def each_side(slot, k, act):
        for side in (0, 1):
            @pl.when(has("px", side))
            def _(side=side):
                act(lambda d, t: x_copy(slot, d, k, t), side)

            @pl.when(has("pz", side))
            def _(side=side):
                act(lambda d, t: z_copy(slot, d, k, t), side)

            edge = pieces - 1 if side else 0

            @pl.when(jnp.logical_and(has("py", side), k == edge))
            def _(side=side):
                act(lambda d, t: y_copy(slot, d, t), side)

    def send(slot, k):
        each_side(slot, k, lambda copy, side: copy(side, side).start())

    def sent(slot, k):
        each_side(slot, k, lambda copy, side: copy(side, side).wait_send())

    def arrived(slot, k):
        each_side(slot, k, lambda copy, side: copy(1 - side, side).wait_recv())

    def sums_copy(k, rows_of):
        return pltpu.make_async_remote_copy(
            src_ref=sq.at[rows_of], dst_ref=sqr.at[rows_of],
            send_sem=qs.at[k], recv_sem=qr.at[k],
            device_id={"px": 1 - here["px"]}, device_id_type=MESH)

    def each_sum(k, act):
        cut = jnp.bool_(False)
        for e in cut_pieces(rows, pieces):
            cut = jnp.logical_or(cut, k == e)

        @pl.when(jnp.logical_not(cut))
        def _():
            act(sums_copy(k, span(k)), k * size, size)

        for turn in (0, 1):
            head, foot = left_over(rows, pieces, turn)
            for e in cut_pieces(rows, pieces):
                low, high = max(e * size, head), min((e + 1) * size, rows - foot)
                if high > low:
                    @pl.when(jnp.logical_and(k == e, here["py"] % 2 == turn))
                    def _(e=e, low=low, high=high):
                        act(sums_copy(e, pl.ds(low, high - low)), low, high - low)

    def over_pieces(act):
        def one(p, carry):
            act(piece(p))
            return carry
        lax.fori_loop(0, pieces, one, 0)

    barrier = pltpu.get_barrier_semaphore()
    count = 0
    for name in names:
        for side in (0, 1):
            there = has(name, side)
            count = count + there.astype(jnp.int32)

            @pl.when(there)
            def _(name=name, side=side):
                pl.semaphore_signal(
                    barrier, inc=1, device_id=beside(name, side), device_id_type=MESH)

    over_pieces(lambda k: load_copy(0, k).start())

    def load_rest(k):
        load_copy(1, k).start()
        load_copy(2, k).start()

    over_pieces(load_rest)

    pl.semaphore_wait(barrier, count)

    def first_send(k):
        load_copy(0, k).wait()
        send(0, k)

    over_pieces(first_send)

    for side in (0, 1):
        for slot in (0, 1):
            @pl.when(jnp.logical_not(has("py", side)))
            def _(side=side, slot=slot):
                u[slot, rows + 1 if side else 0, 1:width + 1] = jnp.zeros(
                    (width, height, lanes), jnp.float32)

            @pl.when(jnp.logical_not(has("px", side)))
            def _(side=side, slot=slot):
                def clear(r, carry):
                    u[slot, r + 1, width + 1 if side else 0] = jnp.zeros(
                        (height, lanes), jnp.float32)
                    return carry
                lax.fori_loop(0, rows, clear, 0)

            @pl.when(jnp.logical_not(has("pz", side)))
            def _(side=side, slot=slot):
                def clear(r, carry):
                    zh[slot, side, r] = jnp.zeros((width, 1, lanes), jnp.float32)
                    return carry
                lax.fori_loop(0, rows, clear, 0)

    level = lax.broadcasted_iota(jnp.int32, (width, height, lanes), 1)

    for step in range(1, STEPS + 1):
        old, new = (step - 1) % 2, step % 2

        def row(r, old, new, final):
            centre = u[old, r + 1, 1:width + 1]
            below = jnp.where(
                level == 0, zh[old, 0, r], pltpu.roll(centre, 1, axis=1))
            above = jnp.where(
                level == height - 1, zh[old, 1, r], pltpu.roll(centre, height - 1, axis=1))
            spread = (
                u[old, r, 1:width + 1]
                + u[old, r + 2, 1:width + 1]
                + u[old, r + 1, 0:width]
                + u[old, r + 1, 2:width + 2]
                + below
                + above
                - 6.0 * centre
            )
            value = centre + c[r] * spread + s[r]
            if final:
                s[r] = value
            else:
                u[new, r + 1, 1:width + 1] = value
            if final and pair:
                mean = jnp.sum(value, axis=0) * (1.0 / width)
                apart = value - mean[None]
                sq[r, 0] = mean
                sq[r, 1] = jnp.sum(apart * apart, axis=0)

        def sweep(k, step=step, old=old, new=new):
            if step == 1:
                load_copy(1, k).wait()
                load_copy(2, k).wait()
            arrived(old, k)
            if 2 <= step < STEPS:
                sent(new, k)

            def one(i, carry):
                row(k * size + i, old, new, step == STEPS)
                return carry
            lax.fori_loop(0, size, one, 0)
            if step < STEPS:
                send(new, k)
            elif pair:
                each_sum(k, lambda copy, first, count: copy.start())

        over_pieces(sweep)

    def finish(copy, first, count):
        copy.wait_recv()

        def one(i, carry):
            r = first + i
            c[r] = normalise(s[r], sq[r], sqr[r])
            return carry
        lax.fori_loop(0, count, one, 0)

    def close(k):
        for slot in sorted({(STEPS - 1) % 2, (STEPS - 2) % 2}):
            sent(slot, k)
        if pair:
            each_sum(k, lambda copy, first, count: copy.wait_send())

    if pair:
        over_pieces(lambda k: each_sum(k, finish))
    over_pieces(close)


def copy_all(copies):
    for copy in copies:
        copy.start()
    for copy in copies:
        copy.wait()


def put_out(pieces, count, *refs):
    held, out, done = refs[:count], refs[count:2 * count], refs[-1]
    size = held[0].shape[0] // pieces
    copy_all([
        pltpu.make_async_copy(
            held[i].at[pl.ds(k * size, size)], out[i].at[pl.ds(k * size, size)], done.at[i, k])
        for k in range(pieces)
        for i in range(count)
    ])


def put_most(pieces, result, end, result_out, end_out, mark, done):
    rows = end.shape[0]
    size = rows // pieces
    mark[...] = jnp.zeros(mark.shape, mark.dtype)
    for turn in (0, 1):
        @pl.when(lax.axis_index("py") % 2 == turn)
        def _(turn=turn):
            head, foot = left_over(rows, pieces, turn)
            copies = []
            for k in range(pieces):
                whole = pl.ds(k * size, size)
                copies.append(pltpu.make_async_copy(
                    end.at[whole], end_out.at[whole], done.at[0, k]))
                low, high = max(k * size, head), min((k + 1) * size, rows - foot)
                if high > low:
                    part = pl.ds(low, high - low)
                    copies.append(pltpu.make_async_copy(
                        result.at[part], result_out.at[part], done.at[1, k]))
            copy_all(copies)


def left_parts(rows, pieces, turn):
    size = rows // pieces
    head, foot = left_over(rows, pieces, turn)
    parts = [(rows - foot + i, head + i, min(size, foot - i)) for i in range(0, foot, size)]
    low = head
    while low > 0:
        count = min(size // 2, max(low // 2, size // 8, 1))
        low -= count
        parts.append((low, low, count))
    return parts


def exchange_rest(pieces, sums, end, mark, out, other, sent, got):
    rows = end.shape[0]
    partner = {"px": 1 - lax.axis_index("px")}
    for turn in (0, 1):
        parts = left_parts(rows, pieces, turn)
        if not parts:
            continue

        @pl.when(lax.axis_index("py") % 2 == turn)
        def _(parts=parts):
            barrier = pltpu.get_barrier_semaphore()
            pl.semaphore_signal(barrier, inc=1, device_id=partner, device_id_type=MESH)
            pl.semaphore_wait(barrier, 1)
            copies = [
                pltpu.make_async_remote_copy(
                    src_ref=sums.at[pl.ds(row, count)], dst_ref=other.at[pl.ds(at, count)],
                    send_sem=sent.at[n], recv_sem=got.at[n],
                    device_id=partner, device_id_type=MESH)
                for n, (row, at, count) in enumerate(parts)
            ]
            for copy in copies:
                copy.start()
            for copy, (row, at, count) in zip(copies, parts):
                copy.wait_recv()

                def one(i, carry, row=row, at=at):
                    out[at + i] = normalise(end[row + i], sums[row + i], other[at + i])
                    return carry
                lax.fori_loop(0, count, one, 0)
            for copy in copies:
                copy.wait_send()


def put_rest(pieces, rest, result, result_out, done):
    rows = result.shape[0]
    for turn in (0, 1):
        @pl.when(lax.axis_index("py") % 2 == turn)
        def _(turn=turn):
            head, foot = left_over(rows, pieces, turn)
            pairs = [((rows - foot, head), foot), ((0, 0), head)]
            copy_all([
                pltpu.make_async_copy(
                    rest.at[pl.ds(at, count)], result_out.at[pl.ds(row, count)], done.at[n])
                for n, ((row, at), count) in enumerate(pairs) if count
            ])


def body(starting_state, scaled_conductivity, scaled_heat_supply):
    rows, width, height, lanes = starting_state.shape
    pieces = next(n for n in (8, 4, 2) if rows % n == 0)
    pair = lax.axis_size("px") == 2
    dma = pltpu.SemaphoreType.DMA
    block = jax.ShapeDtypeStruct(starting_state.shape, jnp.float32)
    field = pltpu.VMEM((rows, width, height, lanes), jnp.float32)
    sums = pltpu.VMEM((rows, 2, height, lanes), jnp.float32)
    here, there = pl.BlockSpec(memory_space=pltpu.VMEM), pl.BlockSpec(memory_space=pl.ANY)
    scratch = [
        pltpu.VMEM((2, rows + 2, width + 2, height, lanes), jnp.float32),
        pltpu.VMEM((2, 2, rows, width, 1, lanes), jnp.float32),
    ]
    scratch += [sums] if pair else [field]
    scratch += [
        dma((3, pieces)),
        dma((2, 2, pieces)), dma((2, 2, pieces)),
        dma((2, 2)), dma((2, 2)),
        dma((2, 2, pieces)), dma((2, 2, pieces)),
    ]
    scratch += [dma((pieces,)), dma((pieces,))] if pair else []
    made = (field, field, sums) if pair else (field,)
    outputs = pl.pallas_call(
        functools.partial(kernel, pieces, pair),
        out_shape=made,
        in_specs=[there] * 3,
        out_specs=(here,) * len(made),
        scratch_shapes=scratch,
        compiler_params=pltpu.CompilerParams(
            collective_id=0, has_side_effects=True, vmem_limit_bytes=(34 if pair else 40) * 1024 * 1024),
    )(starting_state, scaled_conductivity, scaled_heat_supply)
    if pair:
        held, end, kept = outputs
        result, end_out, mark = pl.pallas_call(
            functools.partial(put_most, pieces),
            out_shape=(block, block, pltpu.VMEM((8, 128), jnp.float32)),
            in_specs=[here] * 2,
            out_specs=(there, there, here),
            scratch_shapes=[dma((2, pieces))],
            compiler_params=pltpu.CompilerParams(vmem_limit_bytes=1024 * 1024),
        )(held, end)
        most = max(sum(left_over(rows, pieces, turn)) for turn in (0, 1))
        parts = max(len(left_parts(rows, pieces, turn)) for turn in (0, 1))
        rest = pl.pallas_call(
            functools.partial(exchange_rest, pieces),
            out_shape=pltpu.VMEM((most, width, height, lanes), jnp.float32),
            in_specs=[here] * 3,
            out_specs=here,
            scratch_shapes=[
                pltpu.VMEM((most, 2, height, lanes), jnp.float32), dma((parts,)), dma((parts,))],
            compiler_params=pltpu.CompilerParams(
                collective_id=1, has_side_effects=True, vmem_limit_bytes=4 * 1024 * 1024),
        )(kept, end, mark)
        result = pl.pallas_call(
            functools.partial(put_rest, pieces),
            out_shape=block,
            in_specs=[here, there],
            out_specs=there,
            scratch_shapes=[dma((2,))],
            input_output_aliases={1: 0},
            compiler_params=pltpu.CompilerParams(vmem_limit_bytes=1024 * 1024),
        )(rest, result)
        return result, end_out
    outputs = pl.pallas_call(
        functools.partial(put_out, pieces, len(outputs)),
        out_shape=(block,) * len(outputs),
        in_specs=[here] * len(outputs),
        out_specs=(there,) * len(outputs),
        scratch_shapes=[dma((len(outputs), pieces))],
        compiler_params=pltpu.CompilerParams(vmem_limit_bytes=1024 * 1024),
    )(*outputs)
    (end,) = outputs
    line = width * lax.axis_size("px")
    guess = 1.0
    moved = end - guess
    totals, squares = lax.psum(
        (jnp.sum(moved, axis=1, keepdims=True), jnp.sum(moved * moved, axis=1, keepdims=True)), "px"
    )
    row_average = guess + totals / line
    line_variance = squares / line - totals / line * (totals / line)
    return ((end - row_average) * lax.rsqrt(line_variance + 0.0001), end)


def solution(mesh):
    placed = P("py", "px", "pz", None)
    return jax.shard_map(
        body,
        mesh=mesh,
        in_specs=(placed, placed, placed),
        out_specs=(placed, placed),
        check_vma=False,
    )
```

```python
import functools

import jax
import jax.numpy as jnp
from jax import lax
from jax.experimental import pallas as pl
from jax.experimental.pallas import tpu as pltpu
from jax.sharding import PartitionSpec as P

STEPS = 4
MESH = pl.DeviceIdType.MESH


def left_over(rows, pieces, turn):
    size = rows // pieces
    return (size, size) if turn == 1 else (0, 0)


def cut_pieces(rows, pieces):
    size = rows // pieces
    cut = set()
    for turn in (0, 1):
        head, foot = left_over(rows, pieces, turn)
        cut |= {k for k in range(pieces) if k * size < head or (k + 1) * size > rows - foot}
    return sorted(cut)


def normalise(mine, sums, others):
    width = mine.shape[0]
    gap = sums[0] - others[0]
    mean = 0.5 * (sums[0] + others[0])
    variance = (sums[1] + others[1]) * (0.5 / width) + 0.25 * gap * gap
    return (mine - mean[None]) * lax.rsqrt(variance + 0.0001)[None]


def kernel(pieces, pair, *refs):
    if pair:
        (u_in, c_in, s_in, c, s, sq, u, zh, sqr,
         load, xs, xr, ys, yr, zs, zr, qs, qr) = refs
    else:
        (u_in, c_in, s_in, s, u, zh, c,
         load, xs, xr, ys, yr, zs, zr) = refs
    rows, width, height, lanes = c.shape
    size = rows // pieces
    half = pieces // 2

    names = ("py", "px", "pz")
    here = {name: lax.axis_index(name) for name in names}
    last = {name: lax.axis_size(name) - 1 for name in names}

    def has(name, side):
        return here[name] > 0 if side == 0 else here[name] < last[name]

    def beside(name, side):
        return {name: here[name] + (2 * side - 1)}

    def piece(p):
        odd = p % 2
        return half + (p // 2) * (1 - 2 * odd) - odd

    def span(k, pad=0):
        return pl.ds(k * size + pad, size)

    inner = pl.ds(1, width)

    def load_copy(which, k):
        if which == 0:
            return pltpu.make_async_copy(
                u_in.at[span(k)], u.at[0, span(k, 1), inner], load.at[0, k])
        src, dst = ((c_in, c), (s_in, s))[which - 1]
        return pltpu.make_async_copy(src.at[span(k)], dst.at[span(k)], load.at[which, k])

    def x_copy(slot, side, k, to, first=False):
        inside = u_in.at[span(k), pl.ds(width - 1 if side else 0, 1)]
        return pltpu.make_async_remote_copy(
            src_ref=inside if first else u.at[slot, span(k, 1), pl.ds(width if side else 1, 1)],
            dst_ref=u.at[slot, span(k, 1), pl.ds(0 if side else width + 1, 1)],
            send_sem=xs.at[slot, side, k], recv_sem=xr.at[slot, 1 - side, k],
            device_id=beside("px", to), device_id_type=MESH)

    def z_copy(slot, side, k, to):
        return pltpu.make_async_remote_copy(
            src_ref=u.at[slot, span(k, 1), inner, pl.ds(height - 1 if side else 0, 1)],
            dst_ref=zh.at[slot, 1 - side, span(k)],
            send_sem=zs.at[slot, side, k], recv_sem=zr.at[slot, 1 - side, k],
            device_id=beside("pz", to), device_id_type=MESH)

    def y_copy(slot, side, to):
        return pltpu.make_async_remote_copy(
            src_ref=u.at[slot, pl.ds(rows if side else 1, 1), inner],
            dst_ref=u.at[slot, pl.ds(0 if side else rows + 1, 1), inner],
            send_sem=ys.at[slot, side], recv_sem=yr.at[slot, 1 - side],
            device_id=beside("py", to), device_id_type=MESH)

    def each_side(slot, k, act, x=True, rest=(0, 1), met=False):
        for side in (0, 1):
            if x:
                @pl.when(has("px", side))
                def _(side=side):
                    act(lambda d, t: x_copy(slot, d, k, t), side)

            if side not in rest:
                continue
            beyond = has("pz", side)
            if met and side == 1:
                beyond = jnp.logical_and(beyond, k != half)

            @pl.when(beyond)
            def _(side=side):
                act(lambda d, t: z_copy(slot, d, k, t), side)

            if met and side == 1:
                continue
            edge = pieces - 1 if side else 0

            @pl.when(jnp.logical_and(has("py", side), k == edge))
            def _(side=side):
                act(lambda d, t: y_copy(slot, d, t), side)

    def send(slot, k):
        each_side(slot, k, lambda copy, side: copy(side, side).start())

    def sent(slot, k):
        each_side(slot, k, lambda copy, side: copy(side, side).wait_send())

    def arrived(slot, k, met):
        each_side(slot, k, lambda copy, side: copy(1 - side, side).wait_recv(), met=met)

    def sums_copy(k, rows_of):
        return pltpu.make_async_remote_copy(
            src_ref=sq.at[rows_of], dst_ref=sqr.at[rows_of],
            send_sem=qs.at[k], recv_sem=qr.at[k],
            device_id={"px": 1 - here["px"]}, device_id_type=MESH)

    def each_sum(k, act):
        cut = jnp.bool_(False)
        for e in cut_pieces(rows, pieces):
            cut = jnp.logical_or(cut, k == e)

        @pl.when(jnp.logical_not(cut))
        def _():
            act(sums_copy(k, span(k)), k * size, size)

        for turn in (0, 1):
            head, foot = left_over(rows, pieces, turn)
            for e in cut_pieces(rows, pieces):
                low, high = max(e * size, head), min((e + 1) * size, rows - foot)
                if high > low:
                    @pl.when(jnp.logical_and(k == e, here["py"] % 2 == turn))
                    def _(e=e, low=low, high=high):
                        act(sums_copy(e, pl.ds(low, high - low)), low, high - low)

    def over_pieces(act):
        def one(p, carry):
            act(piece(p))
            return carry
        lax.fori_loop(0, pieces, one, 0)

    load_copy(0, half).start()
    barrier = pltpu.get_barrier_semaphore()
    count = 0
    for name, side in (("px", 0), ("px", 1), ("pz", 1), ("py", 1)):
        there = has(name, side)
        count = count + has(name, side if name == "px" else 0).astype(jnp.int32)

        @pl.when(there)
        def _(name=name, side=side):
            pl.semaphore_signal(
                barrier, inc=1, device_id=beside(name, side), device_id_type=MESH)

    def after_first(act):
        def one(p, carry):
            act(piece(p))
            return carry
        lax.fori_loop(1, pieces, one, 0)

    def start(copy, side):
        copy(side, side).start()

    def first_x(k):
        load_copy(0, k).wait()
        each_side(0, k, start, rest=())

    def load_rest(k):
        load_copy(1, k).start()
        load_copy(2, k).start()

    pl.semaphore_wait(barrier, count)
    for side in (0, 1):
        @pl.when(has("px", side))
        def _(side=side):
            x_copy(0, side, half, side, first=True).start()
    after_first(lambda k: load_copy(0, k).start())
    load_copy(0, half).wait()
    after_first(first_x)
    over_pieces(load_rest)
    over_pieces(lambda k: each_side(0, k, start, x=False, rest=(0,)))

    @pl.when(has("pz", 1))
    def _():
        z_copy(0, 0, half, 1).wait_recv()
        over_pieces(lambda k: z_copy(0, 1, k, 1).start())

    @pl.when(has("py", 1))
    def _():
        y_copy(0, 0, 1).wait_recv()
        y_copy(0, 1, 1).start()

    for side in (0, 1):
        for slot in (0, 1):
            @pl.when(jnp.logical_not(has("py", side)))
            def _(side=side, slot=slot):
                u[slot, rows + 1 if side else 0, 1:width + 1] = jnp.zeros(
                    (width, height, lanes), jnp.float32)

            @pl.when(jnp.logical_not(has("px", side)))
            def _(side=side, slot=slot):
                def clear(r, carry):
                    u[slot, r + 1, width + 1 if side else 0] = jnp.zeros(
                        (height, lanes), jnp.float32)
                    return carry
                lax.fori_loop(0, rows, clear, 0)

            @pl.when(jnp.logical_not(has("pz", side)))
            def _(side=side, slot=slot):
                def clear(r, carry):
                    zh[slot, side, r] = jnp.zeros((width, 1, lanes), jnp.float32)
                    return carry
                lax.fori_loop(0, rows, clear, 0)

    level = lax.broadcasted_iota(jnp.int32, (width, height, lanes), 1)

    for step in range(1, STEPS + 1):
        old, new = (step - 1) % 2, step % 2

        def row(r, old, new, final):
            centre = u[old, r + 1, 1:width + 1]
            below = jnp.where(
                level == 0, zh[old, 0, r], pltpu.roll(centre, 1, axis=1))
            above = jnp.where(
                level == height - 1, zh[old, 1, r], pltpu.roll(centre, height - 1, axis=1))
            spread = (
                u[old, r, 1:width + 1]
                + u[old, r + 2, 1:width + 1]
                + u[old, r + 1, 0:width]
                + u[old, r + 1, 2:width + 2]
                + below
                + above
                - 6.0 * centre
            )
            value = centre + c[r] * spread + s[r]
            if final:
                s[r] = value
            else:
                u[new, r + 1, 1:width + 1] = value
            if final and pair:
                mean = jnp.sum(value, axis=0) * (1.0 / width)
                apart = value - mean[None]
                sq[r, 0] = mean
                sq[r, 1] = jnp.sum(apart * apart, axis=0)

        def sweep(k, step=step, old=old, new=new):
            if step == 1:
                load_copy(1, k).wait()
                load_copy(2, k).wait()
            arrived(old, k, step == 1)
            if 2 <= step < STEPS:
                sent(new, k)

            def one(i, carry):
                row(k * size + i, old, new, step == STEPS)
                return carry
            lax.fori_loop(0, size, one, 0)
            if step < STEPS:
                send(new, k)
            elif pair:
                each_sum(k, lambda copy, first, count: copy.start())

        over_pieces(sweep)

    def finish(copy, first, count):
        copy.wait_recv()

        def one(i, carry):
            r = first + i
            c[r] = normalise(s[r], sq[r], sqr[r])
            return carry
        lax.fori_loop(0, count, one, 0)

    def close(k):
        for slot in sorted({(STEPS - 1) % 2, (STEPS - 2) % 2}):
            sent(slot, k)
        if pair:
            each_sum(k, lambda copy, first, count: copy.wait_send())

    if pair:
        over_pieces(lambda k: each_sum(k, finish))
    over_pieces(close)


def copy_all(copies):
    for copy in copies:
        copy.start()
    for copy in copies:
        copy.wait()


def put_out(pieces, count, *refs):
    held, out, done = refs[:count], refs[count:2 * count], refs[-1]
    size = held[0].shape[0] // pieces
    copy_all([
        pltpu.make_async_copy(
            held[i].at[pl.ds(k * size, size)], out[i].at[pl.ds(k * size, size)], done.at[i, k])
        for k in range(pieces)
        for i in range(count)
    ])


def put_most(pieces, result, end, result_out, end_out, mark, done):
    rows = end.shape[0]
    size = rows // pieces
    mark[...] = jnp.zeros(mark.shape, mark.dtype)
    for turn in (0, 1):
        @pl.when(lax.axis_index("py") % 2 == turn)
        def _(turn=turn):
            head, foot = left_over(rows, pieces, turn)
            copies = []
            for k in range(pieces):
                whole = pl.ds(k * size, size)
                copies.append(pltpu.make_async_copy(
                    end.at[whole], end_out.at[whole], done.at[0, k]))
                low, high = max(k * size, head), min((k + 1) * size, rows - foot)
                if high > low:
                    part = pl.ds(low, high - low)
                    copies.append(pltpu.make_async_copy(
                        result.at[part], result_out.at[part], done.at[1, k]))
            copy_all(copies)


def left_parts(rows, pieces, turn):
    size = rows // pieces
    head, foot = left_over(rows, pieces, turn)
    parts = [(rows - foot + i, head + i, min(size, foot - i)) for i in range(0, foot, size)]
    low = head
    while low > 0:
        count = min(size // 2, max(low // 2, size // 8, 1))
        low -= count
        parts.append((low, low, count))
    return parts


def exchange_rest(pieces, sums, end, mark, out, other, sent, got):
    rows = end.shape[0]
    partner = {"px": 1 - lax.axis_index("px")}
    for turn in (0, 1):
        parts = left_parts(rows, pieces, turn)
        if not parts:
            continue

        @pl.when(lax.axis_index("py") % 2 == turn)
        def _(parts=parts):
            barrier = pltpu.get_barrier_semaphore()
            pl.semaphore_signal(barrier, inc=1, device_id=partner, device_id_type=MESH)
            pl.semaphore_wait(barrier, 1)
            copies = [
                pltpu.make_async_remote_copy(
                    src_ref=sums.at[pl.ds(row, count)], dst_ref=other.at[pl.ds(at, count)],
                    send_sem=sent.at[n], recv_sem=got.at[n],
                    device_id=partner, device_id_type=MESH)
                for n, (row, at, count) in enumerate(parts)
            ]
            for copy in copies:
                copy.start()
            for copy, (row, at, count) in zip(copies, parts):
                copy.wait_recv()

                def one(i, carry, row=row, at=at):
                    out[at + i] = normalise(end[row + i], sums[row + i], other[at + i])
                    return carry
                lax.fori_loop(0, count, one, 0)
            for copy in copies:
                copy.wait_send()


def put_rest(pieces, rest, result, result_out, done):
    rows = result.shape[0]
    for turn in (0, 1):
        @pl.when(lax.axis_index("py") % 2 == turn)
        def _(turn=turn):
            head, foot = left_over(rows, pieces, turn)
            pairs = [((rows - foot, head), foot), ((0, 0), head)]
            copy_all([
                pltpu.make_async_copy(
                    rest.at[pl.ds(at, count)], result_out.at[pl.ds(row, count)], done.at[n])
                for n, ((row, at), count) in enumerate(pairs) if count
            ])


def body(starting_state, scaled_conductivity, scaled_heat_supply):
    rows, width, height, lanes = starting_state.shape
    pieces = next(n for n in (8, 4, 2) if rows % n == 0)
    pair = lax.axis_size("px") == 2
    dma = pltpu.SemaphoreType.DMA
    block = jax.ShapeDtypeStruct(starting_state.shape, jnp.float32)
    field = pltpu.VMEM((rows, width, height, lanes), jnp.float32)
    sums = pltpu.VMEM((rows, 2, height, lanes), jnp.float32)
    here, there = pl.BlockSpec(memory_space=pltpu.VMEM), pl.BlockSpec(memory_space=pl.ANY)
    scratch = [
        pltpu.VMEM((2, rows + 2, width + 2, height, lanes), jnp.float32),
        pltpu.VMEM((2, 2, rows, width, 1, lanes), jnp.float32),
    ]
    scratch += [sums] if pair else [field]
    scratch += [
        dma((3, pieces)),
        dma((2, 2, pieces)), dma((2, 2, pieces)),
        dma((2, 2)), dma((2, 2)),
        dma((2, 2, pieces)), dma((2, 2, pieces)),
    ]
    scratch += [dma((pieces,)), dma((pieces,))] if pair else []
    made = (field, field, sums) if pair else (field,)
    outputs = pl.pallas_call(
        functools.partial(kernel, pieces, pair),
        out_shape=made,
        in_specs=[there] * 3,
        out_specs=(here,) * len(made),
        scratch_shapes=scratch,
        compiler_params=pltpu.CompilerParams(
            collective_id=0, has_side_effects=True, vmem_limit_bytes=(34 if pair else 40) * 1024 * 1024),
    )(starting_state, scaled_conductivity, scaled_heat_supply)
    if pair:
        held, end, kept = outputs
        result, end_out, mark = pl.pallas_call(
            functools.partial(put_most, pieces),
            out_shape=(block, block, pltpu.VMEM((8, 128), jnp.float32)),
            in_specs=[here] * 2,
            out_specs=(there, there, here),
            scratch_shapes=[dma((2, pieces))],
            compiler_params=pltpu.CompilerParams(vmem_limit_bytes=1024 * 1024),
        )(held, end)
        most = max(sum(left_over(rows, pieces, turn)) for turn in (0, 1))
        parts = max(len(left_parts(rows, pieces, turn)) for turn in (0, 1))
        rest = pl.pallas_call(
            functools.partial(exchange_rest, pieces),
            out_shape=pltpu.VMEM((most, width, height, lanes), jnp.float32),
            in_specs=[here] * 3,
            out_specs=here,
            scratch_shapes=[
                pltpu.VMEM((most, 2, height, lanes), jnp.float32), dma((parts,)), dma((parts,))],
            compiler_params=pltpu.CompilerParams(
                collective_id=1, has_side_effects=True, vmem_limit_bytes=4 * 1024 * 1024),
        )(kept, end, mark)
        result = pl.pallas_call(
            functools.partial(put_rest, pieces),
            out_shape=block,
            in_specs=[here, there],
            out_specs=there,
            scratch_shapes=[dma((2,))],
            input_output_aliases={1: 0},
            compiler_params=pltpu.CompilerParams(vmem_limit_bytes=1024 * 1024),
        )(rest, result)
        return result, end_out
    outputs = pl.pallas_call(
        functools.partial(put_out, pieces, len(outputs)),
        out_shape=(block,) * len(outputs),
        in_specs=[here] * len(outputs),
        out_specs=(there,) * len(outputs),
        scratch_shapes=[dma((len(outputs), pieces))],
        compiler_params=pltpu.CompilerParams(vmem_limit_bytes=1024 * 1024),
    )(*outputs)
    (end,) = outputs
    line = width * lax.axis_size("px")
    guess = 1.0
    moved = end - guess
    totals, squares = lax.psum(
        (jnp.sum(moved, axis=1, keepdims=True), jnp.sum(moved * moved, axis=1, keepdims=True)), "px"
    )
    row_average = guess + totals / line
    line_variance = squares / line - totals / line * (totals / line)
    return ((end - row_average) * lax.rsqrt(line_variance + 0.0001), end)


def solution(mesh):
    placed = P("py", "px", "pz", None)
    return jax.shard_map(
        body,
        mesh=mesh,
        in_specs=(placed, placed, placed),
        out_specs=(placed, placed),
        check_vma=False,
    )
```

```python
import functools

import jax
import jax.numpy as jnp
from jax import lax
from jax.experimental import pallas as pl
from jax.experimental.pallas import tpu as pltpu
from jax.sharding import PartitionSpec as P

STEPS = 4
MESH = pl.DeviceIdType.MESH


def left_over(rows, pieces, turn):
    size = rows // pieces
    return (size, size) if turn == 1 else (0, 0)


def cut_pieces(rows, pieces):
    size = rows // pieces
    cut = set()
    for turn in (0, 1):
        head, foot = left_over(rows, pieces, turn)
        cut |= {k for k in range(pieces) if k * size < head or (k + 1) * size > rows - foot}
    return sorted(cut)


def normalise(mine, sums, others):
    width = mine.shape[0]
    gap = sums[0] - others[0]
    mean = 0.5 * (sums[0] + others[0])
    variance = (sums[1] + others[1]) * (0.5 / width) + 0.25 * gap * gap
    return (mine - mean[None]) * lax.rsqrt(variance + 0.0001)[None]


def kernel(pieces, pair, *refs):
    if pair:
        (u_in, c_in, s_in, c, s, sq, u, zh, sqr,
         load, xs, xr, ys, yr, zs, zr, qs, qr) = refs
    else:
        (u_in, c_in, s_in, s, u, zh, c,
         load, xs, xr, ys, yr, zs, zr) = refs
    rows, width, height, lanes = c.shape
    size = rows // pieces
    half = pieces // 2

    names = ("py", "px", "pz")
    here = {name: lax.axis_index(name) for name in names}
    last = {name: lax.axis_size(name) - 1 for name in names}

    def has(name, side):
        return here[name] > 0 if side == 0 else here[name] < last[name]

    def beside(name, side):
        return {name: here[name] + (2 * side - 1)}

    def piece(p):
        odd = p % 2
        return half + (p // 2) * (1 - 2 * odd) - odd

    def span(k, pad=0):
        return pl.ds(k * size + pad, size)

    inner = pl.ds(1, width)

    def load_copy(which, k):
        if which == 0:
            return pltpu.make_async_copy(
                u_in.at[span(k)], u.at[0, span(k, 1), inner], load.at[0, k])
        src, dst = ((c_in, c), (s_in, s))[which - 1]
        return pltpu.make_async_copy(src, dst, load.at[1, which - 1])

    def x_copy(slot, side, k, to, first=False):
        inside = u_in.at[span(k), pl.ds(width - 1 if side else 0, 1)]
        return pltpu.make_async_remote_copy(
            src_ref=inside if first else u.at[slot, span(k, 1), pl.ds(width if side else 1, 1)],
            dst_ref=u.at[slot, span(k, 1), pl.ds(0 if side else width + 1, 1)],
            send_sem=xs.at[slot, 0 if pair else side, k], recv_sem=xr.at[slot, 0 if pair else 1 - side, k],
            device_id=beside("px", to), device_id_type=MESH)

    def z_copy(slot, side, k, to):
        return pltpu.make_async_remote_copy(
            src_ref=u.at[slot, span(k, 1), inner, pl.ds(height - 1 if side else 0, 1)],
            dst_ref=zh.at[slot, 1 - side, span(k)],
            send_sem=zs.at[slot, side, k], recv_sem=zr.at[slot, 1 - side, k],
            device_id=beside("pz", to), device_id_type=MESH)

    def y_copy(slot, side, to):
        return pltpu.make_async_remote_copy(
            src_ref=u.at[slot, pl.ds(rows if side else 1, 1), inner],
            dst_ref=u.at[slot, pl.ds(0 if side else rows + 1, 1), inner],
            send_sem=ys.at[slot, side], recv_sem=yr.at[slot, 1 - side],
            device_id=beside("py", to), device_id_type=MESH)

    def each_side(slot, k, act, x=True, rest=(0, 1), met=False):
        for side in (0, 1):
            if x:
                @pl.when(has("px", side))
                def _(side=side):
                    act(lambda d, t: x_copy(slot, d, k, t), side)

            if side not in rest:
                continue
            beyond = has("pz", side)
            if met and side == 1:
                beyond = jnp.logical_and(beyond, k != half)

            @pl.when(beyond)
            def _(side=side):
                act(lambda d, t: z_copy(slot, d, k, t), side)

            if met and side == 1:
                continue
            edge = pieces - 1 if side else 0

            @pl.when(jnp.logical_and(has("py", side), k == edge))
            def _(side=side):
                act(lambda d, t: y_copy(slot, d, t), side)

    def send(slot, k):
        each_side(slot, k, lambda copy, side: copy(side, side).start())

    def sent(slot, k):
        each_side(slot, k, lambda copy, side: copy(side, side).wait_send())

    def arrived(slot, k, met):
        each_side(slot, k, lambda copy, side: copy(1 - side, side).wait_recv(), met=met)

    def sums_copy(k, rows_of):
        return pltpu.make_async_remote_copy(
            src_ref=sq.at[rows_of], dst_ref=sqr.at[rows_of],
            send_sem=qs.at[k], recv_sem=qr.at[k],
            device_id={"px": 1 - here["px"]}, device_id_type=MESH)

    def each_sum(k, act):
        cut = jnp.bool_(False)
        for e in cut_pieces(rows, pieces):
            cut = jnp.logical_or(cut, k == e)

        @pl.when(jnp.logical_not(cut))
        def _():
            act(sums_copy(k, span(k)), k * size, size)

        for turn in (0, 1):
            head, foot = left_over(rows, pieces, turn)
            for e in cut_pieces(rows, pieces):
                low, high = max(e * size, head), min((e + 1) * size, rows - foot)
                if high > low:
                    @pl.when(jnp.logical_and(k == e, here["py"] % 2 == turn))
                    def _(e=e, low=low, high=high):
                        act(sums_copy(e, pl.ds(low, high - low)), low, high - low)

    def over_pieces(act):
        def one(p, carry):
            act(piece(p))
            return carry
        lax.fori_loop(0, pieces, one, 0)

    load_copy(0, half).start()
    barrier = pltpu.get_barrier_semaphore()
    count = 0
    for name, side in (("px", 0), ("px", 1), ("pz", 1), ("py", 1)):
        there = has(name, side)
        count = count + has(name, side if name == "px" else 0).astype(jnp.int32)

        @pl.when(there)
        def _(name=name, side=side):
            pl.semaphore_signal(
                barrier, inc=1, device_id=beside(name, side), device_id_type=MESH)

    def after_first(act):
        def one(p, carry):
            act(piece(p))
            return carry
        lax.fori_loop(1, pieces, one, 0)

    def start(copy, side):
        copy(side, side).start()

    def first_x(k):
        load_copy(0, k).wait()
        each_side(0, k, start, rest=())

    pl.semaphore_wait(barrier, count)
    for side in (0, 1):
        @pl.when(has("px", side))
        def _(side=side):
            x_copy(0, side, half, side, first=True).start()
    after_first(lambda k: load_copy(0, k).start())
    load_copy(0, half).wait()
    after_first(first_x)
    load_copy(1, 0).start()
    load_copy(2, 0).start()
    over_pieces(lambda k: each_side(0, k, start, x=False, rest=(0,)))

    @pl.when(has("pz", 1))
    def _():
        z_copy(0, 0, half, 1).wait_recv()
        over_pieces(lambda k: z_copy(0, 1, k, 1).start())

    @pl.when(has("py", 1))
    def _():
        y_copy(0, 0, 1).wait_recv()
        y_copy(0, 1, 1).start()

    for side in (0, 1):
        for slot in (0, 1):
            @pl.when(jnp.logical_not(has("py", side)))
            def _(side=side, slot=slot):
                u[slot, rows + 1 if side else 0, 1:width + 1] = jnp.zeros(
                    (width, height, lanes), jnp.float32)

            @pl.when(jnp.logical_not(has("px", side)))
            def _(side=side, slot=slot):
                def clear(r, carry):
                    u[slot, r + 1, width + 1 if side else 0] = jnp.zeros(
                        (height, lanes), jnp.float32)
                    return carry
                lax.fori_loop(0, rows, clear, 0)

            @pl.when(jnp.logical_not(has("pz", side)))
            def _(side=side, slot=slot):
                def clear(r, carry):
                    zh[slot, side, r] = jnp.zeros((width, 1, lanes), jnp.float32)
                    return carry
                lax.fori_loop(0, rows, clear, 0)

    level = lax.broadcasted_iota(jnp.int32, (width, height, lanes), 1)

    for step in range(1, STEPS + 1):
        old, new = (step - 1) % 2, step % 2

        def row(r, old, new, final):
            centre = u[old, r + 1, 1:width + 1]
            below = jnp.where(
                level == 0, zh[old, 0, r], pltpu.roll(centre, 1, axis=1))
            above = jnp.where(
                level == height - 1, zh[old, 1, r], pltpu.roll(centre, height - 1, axis=1))
            spread = (
                u[old, r, 1:width + 1]
                + u[old, r + 2, 1:width + 1]
                + u[old, r + 1, 0:width]
                + u[old, r + 1, 2:width + 2]
                + below
                + above
                - 6.0 * centre
            )
            value = centre + c[r] * spread + s[r]
            if final:
                s[r] = value
            else:
                u[new, r + 1, 1:width + 1] = value
            if final and pair:
                mean = jnp.sum(value, axis=0) * (1.0 / width)
                apart = value - mean[None]
                sq[r, 0] = mean
                sq[r, 1] = jnp.sum(apart * apart, axis=0)

        def sweep(k, step=step, old=old, new=new):
            arrived(old, k, step == 1)
            if 2 <= step < STEPS:
                sent(new, k)

            def one(i, carry):
                row(k * size + i, old, new, step == STEPS)
                return carry
            lax.fori_loop(0, size, one, 0)
            if step < STEPS:
                send(new, k)
            elif pair:
                each_sum(k, lambda copy, first, count: copy.start())

        if step == 1:
            load_copy(1, 0).wait()
            load_copy(2, 0).wait()
        over_pieces(sweep)

    def finish(copy, first, count):
        copy.wait_recv()

        def one(i, carry):
            r = first + i
            c[r] = normalise(s[r], sq[r], sqr[r])
            return carry
        lax.fori_loop(0, count, one, 0)

    def close(k):
        for slot in sorted({(STEPS - 1) % 2, (STEPS - 2) % 2}):
            sent(slot, k)
        if pair:
            each_sum(k, lambda copy, first, count: copy.wait_send())

    if pair:
        over_pieces(lambda k: each_sum(k, finish))
    over_pieces(close)


def copy_all(copies):
    for copy in copies:
        copy.start()
    for copy in copies:
        copy.wait()


def put_out(pieces, count, *refs):
    held, out, done = refs[:count], refs[count:2 * count], refs[-1]
    size = held[0].shape[0] // pieces
    copy_all([
        pltpu.make_async_copy(
            held[i].at[pl.ds(k * size, size)], out[i].at[pl.ds(k * size, size)], done.at[i, k])
        for k in range(pieces)
        for i in range(count)
    ])


def put_most(pieces, result, end, result_out, end_out, mark, done):
    rows = end.shape[0]
    size = rows // pieces
    mark[...] = jnp.zeros(mark.shape, mark.dtype)
    for turn in (0, 1):
        @pl.when(lax.axis_index("py") % 2 == turn)
        def _(turn=turn):
            head, foot = left_over(rows, pieces, turn)
            copies = []
            for k in range(pieces):
                whole = pl.ds(k * size, size)
                copies.append(pltpu.make_async_copy(
                    end.at[whole], end_out.at[whole], done.at[0, k]))
                low, high = max(k * size, head), min((k + 1) * size, rows - foot)
                if high > low:
                    part = pl.ds(low, high - low)
                    copies.append(pltpu.make_async_copy(
                        result.at[part], result_out.at[part], done.at[1, k]))
            copy_all(copies)


def left_parts(rows, pieces, turn):
    size = rows // pieces
    head, foot = left_over(rows, pieces, turn)
    parts = [(rows - foot + i, head + i, min(size, foot - i)) for i in range(0, foot, size)]
    low = head
    while low > 0:
        count = min(low, size // 2, max(low // 2, size // 8, 1))
        low -= count
        parts.append((low, low, count))
    return parts


def exchange_rest(pieces, sums, end, mark, out, other, sent, got):
    rows = end.shape[0]
    partner = {"px": 1 - lax.axis_index("px")}
    for turn in (0, 1):
        parts = left_parts(rows, pieces, turn)
        if not parts:
            continue

        @pl.when(lax.axis_index("py") % 2 == turn)
        def _(parts=parts):
            barrier = pltpu.get_barrier_semaphore()
            pl.semaphore_signal(barrier, inc=1, device_id=partner, device_id_type=MESH)
            pl.semaphore_wait(barrier, 1)
            copies = [
                pltpu.make_async_remote_copy(
                    src_ref=sums.at[pl.ds(row, count)], dst_ref=other.at[pl.ds(at, count)],
                    send_sem=sent.at[n], recv_sem=got.at[n],
                    device_id=partner, device_id_type=MESH)
                for n, (row, at, count) in enumerate(parts)
            ]
            for copy in copies:
                copy.start()
            for copy, (row, at, count) in zip(copies, parts):
                copy.wait_recv()

                def one(i, carry, row=row, at=at):
                    out[at + i] = normalise(end[row + i], sums[row + i], other[at + i])
                    return carry
                lax.fori_loop(0, count, one, 0)
            for copy in copies:
                copy.wait_send()


def put_rest(pieces, rest, result, result_out, done):
    rows = result.shape[0]
    for turn in (0, 1):
        @pl.when(lax.axis_index("py") % 2 == turn)
        def _(turn=turn):
            head, foot = left_over(rows, pieces, turn)
            pairs = [((rows - foot, head), foot), ((0, 0), head)]
            copy_all([
                pltpu.make_async_copy(
                    rest.at[pl.ds(at, count)], result_out.at[pl.ds(row, count)], done.at[n])
                for n, ((row, at), count) in enumerate(pairs) if count
            ])


def body(starting_state, scaled_conductivity, scaled_heat_supply):
    rows, width, height, lanes = starting_state.shape
    pieces = next(n for n in (8, 4, 2) if rows % n == 0)
    pair = lax.axis_size("px") == 2
    dma = pltpu.SemaphoreType.DMA
    block = jax.ShapeDtypeStruct(starting_state.shape, jnp.float32)
    field = pltpu.VMEM((rows, width, height, lanes), jnp.float32)
    sums = pltpu.VMEM((rows, 2, height, lanes), jnp.float32)
    here, there = pl.BlockSpec(memory_space=pltpu.VMEM), pl.BlockSpec(memory_space=pl.ANY)
    scratch = [
        pltpu.VMEM((2, rows + 2, width + 2, height, lanes), jnp.float32),
        pltpu.VMEM((2, 2, rows, width, 1, lanes), jnp.float32),
    ]
    scratch += [sums] if pair else [field]
    scratch += [
        dma((2, pieces)),
        dma((2, 1 if pair else 2, pieces)), dma((2, 1 if pair else 2, pieces)),
        dma((2, 2)), dma((2, 2)),
        dma((2, 2, pieces)), dma((2, 2, pieces)),
    ]
    scratch += [dma((pieces,)), dma((pieces,))] if pair else []
    made = (field, field, sums) if pair else (field,)
    outputs = pl.pallas_call(
        functools.partial(kernel, pieces, pair),
        out_shape=made,
        in_specs=[there] * 3,
        out_specs=(here,) * len(made),
        scratch_shapes=scratch,
        compiler_params=pltpu.CompilerParams(
            collective_id=0, has_side_effects=True, vmem_limit_bytes=(34 if pair else 40) * 1024 * 1024),
    )(starting_state, scaled_conductivity, scaled_heat_supply)
    if pair:
        held, end, kept = outputs
        result, end_out, mark = pl.pallas_call(
            functools.partial(put_most, pieces),
            out_shape=(block, block, pltpu.VMEM((8, 128), jnp.float32)),
            in_specs=[here] * 2,
            out_specs=(there, there, here),
            scratch_shapes=[dma((2, pieces))],
            compiler_params=pltpu.CompilerParams(vmem_limit_bytes=1024 * 1024),
        )(held, end)
        most = max(sum(left_over(rows, pieces, turn)) for turn in (0, 1))
        parts = max(len(left_parts(rows, pieces, turn)) for turn in (0, 1))
        rest = pl.pallas_call(
            functools.partial(exchange_rest, pieces),
            out_shape=pltpu.VMEM((most, width, height, lanes), jnp.float32),
            in_specs=[here] * 3,
            out_specs=here,
            scratch_shapes=[
                pltpu.VMEM((most, 2, height, lanes), jnp.float32), dma((parts,)), dma((parts,))],
            compiler_params=pltpu.CompilerParams(
                collective_id=1, has_side_effects=True, vmem_limit_bytes=4 * 1024 * 1024),
        )(kept, end, mark)
        result = pl.pallas_call(
            functools.partial(put_rest, pieces),
            out_shape=block,
            in_specs=[here, there],
            out_specs=there,
            scratch_shapes=[dma((2,))],
            input_output_aliases={1: 0},
            compiler_params=pltpu.CompilerParams(vmem_limit_bytes=1024 * 1024),
        )(rest, result)
        return result, end_out
    outputs = pl.pallas_call(
        functools.partial(put_out, pieces, len(outputs)),
        out_shape=(block,) * len(outputs),
        in_specs=[here] * len(outputs),
        out_specs=(there,) * len(outputs),
        scratch_shapes=[dma((len(outputs), pieces))],
        compiler_params=pltpu.CompilerParams(vmem_limit_bytes=1024 * 1024),
    )(*outputs)
    (end,) = outputs
    line = width * lax.axis_size("px")
    guess = 1.0
    moved = end - guess
    totals, squares = lax.psum(
        (jnp.sum(moved, axis=1, keepdims=True), jnp.sum(moved * moved, axis=1, keepdims=True)), "px"
    )
    row_average = guess + totals / line
    line_variance = squares / line - totals / line * (totals / line)
    return ((end - row_average) * lax.rsqrt(line_variance + 0.0001), end)


def solution(mesh):
    placed = P("py", "px", "pz", None)
    return jax.shard_map(
        body,
        mesh=mesh,
        in_specs=(placed, placed, placed),
        out_specs=(placed, placed),
        check_vma=False,
    )
```

```python
import functools

import jax
import jax.numpy as jnp
from jax import lax
from jax.experimental import pallas as pl
from jax.experimental.pallas import tpu as pltpu
from jax.sharding import PartitionSpec as P

STEPS = 4
MESH = pl.DeviceIdType.MESH


def left_over(rows, pieces, turn):
    size = rows // pieces
    return (size, size) if turn == 1 else (0, 0)


def cut_pieces(rows, pieces):
    size = rows // pieces
    cut = set()
    for turn in (0, 1):
        head, foot = left_over(rows, pieces, turn)
        cut |= {k for k in range(pieces) if k * size < head or (k + 1) * size > rows - foot}
    return sorted(cut)


def normalise(mine, sums, others):
    width = mine.shape[0]
    gap = sums[0] - others[0]
    mean = 0.5 * (sums[0] + others[0])
    variance = (sums[1] + others[1]) * (0.5 / width) + 0.25 * gap * gap
    return (mine - mean[None]) * lax.rsqrt(variance + 0.0001)[None]


def kernel(pieces, pair, *refs):
    if pair:
        (u_in, c_in, s_in, c, s, sq, u, zh, sqr,
         load, xs, xr, ys, yr, zs, zr, qs, qr) = refs
    else:
        (u_in, c_in, s_in, s, u, zh, c,
         load, xs, xr, ys, yr, zs, zr) = refs
    rows, width, height, lanes = c.shape
    size = rows // pieces
    half = pieces // 2

    names = ("py", "px", "pz")
    here = {name: lax.axis_index(name) for name in names}
    last = {name: lax.axis_size(name) - 1 for name in names}

    def has(name, side):
        return here[name] > 0 if side == 0 else here[name] < last[name]

    def beside(name, side):
        return {name: here[name] + (2 * side - 1)}

    def piece(p):
        odd = p % 2
        return half + (p // 2) * (1 - 2 * odd) - odd

    def span(k, pad=0):
        return pl.ds(k * size + pad, size)

    inner = pl.ds(1, width)

    def load_copy(which, k):
        if which == 0:
            return pltpu.make_async_copy(
                u_in.at[span(k)], u.at[0, span(k, 1), inner], load.at[0, k])
        src, dst = ((c_in, c), (s_in, s))[which - 1]
        return pltpu.make_async_copy(src, dst, load.at[1, which - 1])

    def x_copy(slot, side, k, to, first=False):
        inside = u_in.at[span(k), pl.ds(width - 1 if side else 0, 1)]
        return pltpu.make_async_remote_copy(
            src_ref=inside if first else u.at[slot, span(k, 1), pl.ds(width if side else 1, 1)],
            dst_ref=u.at[slot, span(k, 1), pl.ds(0 if side else width + 1, 1)],
            send_sem=xs.at[slot, 0 if pair else side, k], recv_sem=xr.at[slot, 0 if pair else 1 - side, k],
            device_id=beside("px", to), device_id_type=MESH)

    def z_copy(slot, side, k, to):
        return pltpu.make_async_remote_copy(
            src_ref=u.at[slot, span(k, 1), inner, pl.ds(height - 1 if side else 0, 1)],
            dst_ref=zh.at[slot, 1 - side, span(k)],
            send_sem=zs.at[slot, side, k], recv_sem=zr.at[slot, 1 - side, k],
            device_id=beside("pz", to), device_id_type=MESH)

    def y_copy(slot, side, to):
        return pltpu.make_async_remote_copy(
            src_ref=u.at[slot, pl.ds(rows if side else 1, 1), inner],
            dst_ref=u.at[slot, pl.ds(0 if side else rows + 1, 1), inner],
            send_sem=ys.at[slot, side], recv_sem=yr.at[slot, 1 - side],
            device_id=beside("py", to), device_id_type=MESH)

    def each_side(slot, k, act, x=True, rest=(0, 1), met=False):
        for side in (0, 1):
            if x:
                @pl.when(has("px", side))
                def _(side=side):
                    act(lambda d, t: x_copy(slot, d, k, t), side)

            if side not in rest:
                continue
            beyond = has("pz", side)
            if met and side == 1:
                beyond = jnp.logical_and(beyond, k != half)

            @pl.when(beyond)
            def _(side=side):
                act(lambda d, t: z_copy(slot, d, k, t), side)

            if met and side == 1:
                continue
            edge = pieces - 1 if side else 0

            @pl.when(jnp.logical_and(has("py", side), k == edge))
            def _(side=side):
                act(lambda d, t: y_copy(slot, d, t), side)

    def send(slot, k):
        each_side(slot, k, lambda copy, side: copy(side, side).start())

    def sent(slot, k):
        each_side(slot, k, lambda copy, side: copy(side, side).wait_send())

    def arrived(slot, k, met):
        each_side(slot, k, lambda copy, side: copy(1 - side, side).wait_recv(), met=met)

    def sums_copy(k, rows_of):
        return pltpu.make_async_remote_copy(
            src_ref=sq.at[rows_of], dst_ref=sqr.at[rows_of],
            send_sem=qs.at[k], recv_sem=qr.at[k],
            device_id={"px": 1 - here["px"]}, device_id_type=MESH)

    def each_sum(k, act):
        cut = jnp.bool_(False)
        for e in cut_pieces(rows, pieces):
            cut = jnp.logical_or(cut, k == e)

        @pl.when(jnp.logical_not(cut))
        def _():
            act(sums_copy(k, span(k)), k * size, size)

        for turn in (0, 1):
            head, foot = left_over(rows, pieces, turn)
            for e in cut_pieces(rows, pieces):
                low, high = max(e * size, head), min((e + 1) * size, rows - foot)
                if high > low:
                    @pl.when(jnp.logical_and(k == e, here["py"] % 2 == turn))
                    def _(e=e, low=low, high=high):
                        act(sums_copy(e, pl.ds(low, high - low)), low, high - low)

    def over_pieces(act):
        def one(p, carry):
            act(piece(p))
            return carry
        lax.fori_loop(0, pieces, one, 0)

    barrier = pltpu.get_barrier_semaphore()
    count = 0
    for name, side in (("px", 0), ("px", 1), ("pz", 1), ("py", 1)):
        there = has(name, side)
        count = count + has(name, side if name == "px" else 0).astype(jnp.int32)

        @pl.when(there)
        def _(name=name, side=side):
            pl.semaphore_signal(
                barrier, inc=1, device_id=beside(name, side), device_id_type=MESH)

    def after_first(act):
        def one(p, carry):
            act(piece(p))
            return carry
        lax.fori_loop(1, pieces, one, 0)

    def start(copy, side):
        copy(side, side).start()

    def first_x(k):
        load_copy(0, k).wait()
        each_side(0, k, start, rest=())

    pl.semaphore_wait(barrier, count)
    for side in (0, 1):
        @pl.when(has("px", side))
        def _(side=side):
            x_copy(0, side, half, side, first=True).start()
    over_pieces(lambda k: load_copy(0, k).start())
    load_copy(0, half).wait()
    after_first(first_x)
    load_copy(1, 0).start()
    load_copy(2, 0).start()
    over_pieces(lambda k: each_side(0, k, start, x=False, rest=(0,)))

    @pl.when(has("pz", 1))
    def _():
        z_copy(0, 0, half, 1).wait_recv()
        over_pieces(lambda k: z_copy(0, 1, k, 1).start())

    @pl.when(has("py", 1))
    def _():
        y_copy(0, 0, 1).wait_recv()
        y_copy(0, 1, 1).start()

    for side in (0, 1):
        for slot in (0, 1):
            @pl.when(jnp.logical_not(has("py", side)))
            def _(side=side, slot=slot):
                u[slot, rows + 1 if side else 0, 1:width + 1] = jnp.zeros(
                    (width, height, lanes), jnp.float32)

            @pl.when(jnp.logical_not(has("px", side)))
            def _(side=side, slot=slot):
                def clear(r, carry):
                    u[slot, r + 1, width + 1 if side else 0] = jnp.zeros(
                        (height, lanes), jnp.float32)
                    return carry
                lax.fori_loop(0, rows, clear, 0)

            @pl.when(jnp.logical_not(has("pz", side)))
            def _(side=side, slot=slot):
                def clear(r, carry):
                    zh[slot, side, r] = jnp.zeros((width, 1, lanes), jnp.float32)
                    return carry
                lax.fori_loop(0, rows, clear, 0)

    level = lax.broadcasted_iota(jnp.int32, (width, height, lanes), 1)

    for step in range(1, STEPS + 1):
        old, new = (step - 1) % 2, step % 2

        def row(r, old, new, final):
            centre = u[old, r + 1, 1:width + 1]
            below = jnp.where(
                level == 0, zh[old, 0, r], pltpu.roll(centre, 1, axis=1))
            above = jnp.where(
                level == height - 1, zh[old, 1, r], pltpu.roll(centre, height - 1, axis=1))
            spread = (
                u[old, r, 1:width + 1]
                + u[old, r + 2, 1:width + 1]
                + u[old, r + 1, 0:width]
                + u[old, r + 1, 2:width + 2]
                + below
                + above
                - 6.0 * centre
            )
            value = centre + c[r] * spread + s[r]
            if final:
                s[r] = value
            else:
                u[new, r + 1, 1:width + 1] = value
            if final and pair:
                mean = jnp.sum(value, axis=0) * (1.0 / width)
                apart = value - mean[None]
                sq[r, 0] = mean
                sq[r, 1] = jnp.sum(apart * apart, axis=0)

        def sweep(k, step=step, old=old, new=new):
            arrived(old, k, step == 1)
            if 2 <= step < STEPS:
                sent(new, k)

            def one(i, carry):
                row(k * size + i, old, new, step == STEPS)
                return carry
            lax.fori_loop(0, size, one, 0)
            if step < STEPS:
                send(new, k)
            elif pair:
                each_sum(k, lambda copy, first, count: copy.start())

        if step == 1:
            load_copy(1, 0).wait()
            load_copy(2, 0).wait()
        over_pieces(sweep)

    def finish(copy, first, count):
        copy.wait_recv()

        def one(i, carry):
            r = first + i
            c[r] = normalise(s[r], sq[r], sqr[r])
            return carry
        lax.fori_loop(0, count, one, 0)

    def close(k):
        for slot in sorted({(STEPS - 1) % 2, (STEPS - 2) % 2}):
            sent(slot, k)
        if pair:
            each_sum(k, lambda copy, first, count: copy.wait_send())

    if pair:
        over_pieces(lambda k: each_sum(k, finish))
    over_pieces(close)


def copy_all(copies):
    for copy in copies:
        copy.start()
    for copy in copies:
        copy.wait()


def put_out(pieces, count, *refs):
    held, out, done = refs[:count], refs[count:2 * count], refs[-1]
    size = held[0].shape[0] // pieces
    copy_all([
        pltpu.make_async_copy(
            held[i].at[pl.ds(k * size, size)], out[i].at[pl.ds(k * size, size)], done.at[i, k])
        for k in range(pieces)
        for i in range(count)
    ])


def put_most(pieces, result, end, result_out, end_out, mark, done):
    rows = end.shape[0]
    size = rows // pieces
    mark[...] = jnp.zeros(mark.shape, mark.dtype)
    for turn in (0, 1):
        @pl.when(lax.axis_index("py") % 2 == turn)
        def _(turn=turn):
            head, foot = left_over(rows, pieces, turn)
            copies = []
            for k in range(pieces):
                whole = pl.ds(k * size, size)
                copies.append(pltpu.make_async_copy(
                    end.at[whole], end_out.at[whole], done.at[0, k]))
                low, high = max(k * size, head), min((k + 1) * size, rows - foot)
                if high > low:
                    part = pl.ds(low, high - low)
                    copies.append(pltpu.make_async_copy(
                        result.at[part], result_out.at[part], done.at[1, k]))
            copy_all(copies)


def left_parts(rows, pieces, turn):
    size = rows // pieces
    head, foot = left_over(rows, pieces, turn)
    parts = [(rows - foot + i, head + i, min(size, foot - i)) for i in range(0, foot, size)]
    low = head
    while low > 0:
        count = min(low, size // 2, max(low // 2, size // 8, 1))
        low -= count
        parts.append((low, low, count))
    return parts


def exchange_rest(pieces, sums, end, mark, out, other, sent, got):
    rows = end.shape[0]
    partner = {"px": 1 - lax.axis_index("px")}
    for turn in (0, 1):
        parts = left_parts(rows, pieces, turn)
        if not parts:
            continue

        @pl.when(lax.axis_index("py") % 2 == turn)
        def _(parts=parts):
            barrier = pltpu.get_barrier_semaphore()
            pl.semaphore_signal(barrier, inc=1, device_id=partner, device_id_type=MESH)
            pl.semaphore_wait(barrier, 1)
            copies = [
                pltpu.make_async_remote_copy(
                    src_ref=sums.at[pl.ds(row, count)], dst_ref=other.at[pl.ds(at, count)],
                    send_sem=sent.at[n], recv_sem=got.at[n],
                    device_id=partner, device_id_type=MESH)
                for n, (row, at, count) in enumerate(parts)
            ]
            for copy in copies:
                copy.start()
            for copy, (row, at, count) in zip(copies, parts):
                copy.wait_recv()

                def one(i, carry, row=row, at=at):
                    out[at + i] = normalise(end[row + i], sums[row + i], other[at + i])
                    return carry
                lax.fori_loop(0, count, one, 0)
            for copy in copies:
                copy.wait_send()


def put_rest(pieces, rest, result, result_out, done):
    rows = result.shape[0]
    for turn in (0, 1):
        @pl.when(lax.axis_index("py") % 2 == turn)
        def _(turn=turn):
            head, foot = left_over(rows, pieces, turn)
            pairs = [((rows - foot, head), foot), ((0, 0), head)]
            copy_all([
                pltpu.make_async_copy(
                    rest.at[pl.ds(at, count)], result_out.at[pl.ds(row, count)], done.at[n])
                for n, ((row, at), count) in enumerate(pairs) if count
            ])


def body(starting_state, scaled_conductivity, scaled_heat_supply):
    rows, width, height, lanes = starting_state.shape
    pieces = next(n for n in (8, 4, 2) if rows % n == 0)
    pair = lax.axis_size("px") == 2
    dma = pltpu.SemaphoreType.DMA
    block = jax.ShapeDtypeStruct(starting_state.shape, jnp.float32)
    field = pltpu.VMEM((rows, width, height, lanes), jnp.float32)
    sums = pltpu.VMEM((rows, 2, height, lanes), jnp.float32)
    here, there = pl.BlockSpec(memory_space=pltpu.VMEM), pl.BlockSpec(memory_space=pl.ANY)
    scratch = [
        pltpu.VMEM((2, rows + 2, width + 2, height, lanes), jnp.float32),
        pltpu.VMEM((2, 2, rows, width, 1, lanes), jnp.float32),
    ]
    scratch += [sums] if pair else [field]
    scratch += [
        dma((2, pieces)),
        dma((2, 1 if pair else 2, pieces)), dma((2, 1 if pair else 2, pieces)),
        dma((2, 2)), dma((2, 2)),
        dma((2, 2, pieces)), dma((2, 2, pieces)),
    ]
    scratch += [dma((pieces,)), dma((pieces,))] if pair else []
    made = (field, field, sums) if pair else (field,)
    outputs = pl.pallas_call(
        functools.partial(kernel, pieces, pair),
        out_shape=made,
        in_specs=[there] * 3,
        out_specs=(here,) * len(made),
        scratch_shapes=scratch,
        compiler_params=pltpu.CompilerParams(
            collective_id=0, has_side_effects=True, vmem_limit_bytes=(34 if pair else 40) * 1024 * 1024),
    )(starting_state, scaled_conductivity, scaled_heat_supply)
    if pair:
        held, end, kept = outputs
        result, end_out, mark = pl.pallas_call(
            functools.partial(put_most, pieces),
            out_shape=(block, block, pltpu.VMEM((8, 128), jnp.float32)),
            in_specs=[here] * 2,
            out_specs=(there, there, here),
            scratch_shapes=[dma((2, pieces))],
            compiler_params=pltpu.CompilerParams(vmem_limit_bytes=1024 * 1024),
        )(held, end)
        most = max(sum(left_over(rows, pieces, turn)) for turn in (0, 1))
        parts = max(len(left_parts(rows, pieces, turn)) for turn in (0, 1))
        rest = pl.pallas_call(
            functools.partial(exchange_rest, pieces),
            out_shape=pltpu.VMEM((most, width, height, lanes), jnp.float32),
            in_specs=[here] * 3,
            out_specs=here,
            scratch_shapes=[
                pltpu.VMEM((most, 2, height, lanes), jnp.float32), dma((parts,)), dma((parts,))],
            compiler_params=pltpu.CompilerParams(
                collective_id=1, has_side_effects=True, vmem_limit_bytes=4 * 1024 * 1024),
        )(kept, end, mark)
        result = pl.pallas_call(
            functools.partial(put_rest, pieces),
            out_shape=block,
            in_specs=[here, there],
            out_specs=there,
            scratch_shapes=[dma((2,))],
            input_output_aliases={1: 0},
            compiler_params=pltpu.CompilerParams(vmem_limit_bytes=1024 * 1024),
        )(rest, result)
        return result, end_out
    outputs = pl.pallas_call(
        functools.partial(put_out, pieces, len(outputs)),
        out_shape=(block,) * len(outputs),
        in_specs=[here] * len(outputs),
        out_specs=(there,) * len(outputs),
        scratch_shapes=[dma((len(outputs), pieces))],
        compiler_params=pltpu.CompilerParams(vmem_limit_bytes=1024 * 1024),
    )(*outputs)
    (end,) = outputs
    line = width * lax.axis_size("px")
    guess = 1.0
    moved = end - guess
    totals, squares = lax.psum(
        (jnp.sum(moved, axis=1, keepdims=True), jnp.sum(moved * moved, axis=1, keepdims=True)), "px"
    )
    row_average = guess + totals / line
    line_variance = squares / line - totals / line * (totals / line)
    return ((end - row_average) * lax.rsqrt(line_variance + 0.0001), end)


def solution(mesh):
    placed = P("py", "px", "pz", None)
    return jax.shard_map(
        body,
        mesh=mesh,
        in_specs=(placed, placed, placed),
        out_specs=(placed, placed),
        check_vma=False,
    )
```

```python
import functools

import jax
import jax.numpy as jnp
from jax import lax
from jax.experimental import pallas as pl
from jax.experimental.pallas import tpu as pltpu
from jax.sharding import PartitionSpec as P

STEPS = 4
MESH = pl.DeviceIdType.MESH


def left_over(rows, pieces, turn):
    size = rows // pieces
    return (size, size) if turn == 1 else (0, 0)


def cut_pieces(rows, pieces):
    size = rows // pieces
    cut = set()
    for turn in (0, 1):
        head, foot = left_over(rows, pieces, turn)
        cut |= {k for k in range(pieces) if k * size < head or (k + 1) * size > rows - foot}
    return sorted(cut)


def normalise(mine, sums, others):
    width = mine.shape[0]
    gap = sums[0] - others[0]
    mean = 0.5 * (sums[0] + others[0])
    variance = (sums[1] + others[1]) * (0.5 / width) + 0.25 * gap * gap
    return (mine - mean[None]) * lax.rsqrt(variance + 0.0001)[None]


def kernel(pieces, pair, *refs):
    if pair:
        (u_in, c_in, s_in, c, s, sq, u, zh, sqr,
         load, xs, xr, ys, yr, zs, zr, qs, qr) = refs
    else:
        (u_in, c_in, s_in, s, u, zh, c,
         load, xs, xr, ys, yr, zs, zr) = refs
    rows, width, height, lanes = c.shape
    size = rows // pieces
    half = pieces // 2

    names = ("py", "px", "pz")
    here = {name: lax.axis_index(name) for name in names}
    last = {name: lax.axis_size(name) - 1 for name in names}

    def has(name, side):
        return here[name] > 0 if side == 0 else here[name] < last[name]

    def beside(name, side):
        return {name: here[name] + (2 * side - 1)}

    def piece(p):
        odd = p % 2
        return half + (p // 2) * (1 - 2 * odd) - odd

    def span(k, pad=0):
        return pl.ds(k * size + pad, size)

    inner = pl.ds(1, width)

    def load_copy(which, k):
        if which == 0:
            return pltpu.make_async_copy(
                u_in.at[span(k)], u.at[0, span(k, 1), inner], load.at[0, k])
        src, dst = ((c_in, c), (s_in, s))[which - 1]
        return pltpu.make_async_copy(src, dst, load.at[1, which - 1])

    def x_copy(slot, side, k, to, first=False):
        inside = u_in.at[span(k), pl.ds(width - 1 if side else 0, 1)]
        return pltpu.make_async_remote_copy(
            src_ref=inside if first else u.at[slot, span(k, 1), pl.ds(width if side else 1, 1)],
            dst_ref=u.at[slot, span(k, 1), pl.ds(0 if side else width + 1, 1)],
            send_sem=xs.at[slot, 0 if pair else side, k], recv_sem=xr.at[slot, 0 if pair else 1 - side, k],
            device_id=beside("px", to), device_id_type=MESH)

    def z_copy(slot, side, k, to):
        return pltpu.make_async_remote_copy(
            src_ref=u.at[slot, span(k, 1), inner, pl.ds(height - 1 if side else 0, 1)],
            dst_ref=zh.at[slot, 1 - side, span(k)],
            send_sem=zs.at[slot, side, k], recv_sem=zr.at[slot, 1 - side, k],
            device_id=beside("pz", to), device_id_type=MESH)

    def y_copy(slot, side, to):
        return pltpu.make_async_remote_copy(
            src_ref=u.at[slot, pl.ds(rows if side else 1, 1), inner],
            dst_ref=u.at[slot, pl.ds(0 if side else rows + 1, 1), inner],
            send_sem=ys.at[slot, side], recv_sem=yr.at[slot, 1 - side],
            device_id=beside("py", to), device_id_type=MESH)

    def each_side(slot, k, act, x=True, rest=(0, 1), met=False):
        for side in (0, 1):
            if x:
                @pl.when(has("px", side))
                def _(side=side):
                    act(lambda d, t: x_copy(slot, d, k, t), side)

            if side not in rest:
                continue
            beyond = has("pz", side)
            if met and side == 1:
                beyond = jnp.logical_and(beyond, k != half)

            @pl.when(beyond)
            def _(side=side):
                act(lambda d, t: z_copy(slot, d, k, t), side)

            if rest != (0, 1):
                continue
            edge = pieces - 1 if side else 0
            beyond = jnp.logical_and(has("py", side), k == edge)
            if met:
                beyond = jnp.logical_and(beyond, patient)

            @pl.when(beyond)
            def _(side=side):
                act(lambda d, t: y_copy(slot, d, t), side)

    def send(slot, k):
        each_side(slot, k, lambda copy, side: copy(side, side).start())

    def sent(slot, k):
        each_side(slot, k, lambda copy, side: copy(side, side).wait_send())

    def arrived(slot, k, met):
        each_side(slot, k, lambda copy, side: copy(1 - side, side).wait_recv(), met=met)

    def sums_copy(k, rows_of):
        return pltpu.make_async_remote_copy(
            src_ref=sq.at[rows_of], dst_ref=sqr.at[rows_of],
            send_sem=qs.at[k], recv_sem=qr.at[k],
            device_id={"px": 1 - here["px"]}, device_id_type=MESH)

    def each_sum(k, act):
        cut = jnp.bool_(False)
        for e in cut_pieces(rows, pieces):
            cut = jnp.logical_or(cut, k == e)

        @pl.when(jnp.logical_not(cut))
        def _():
            act(sums_copy(k, span(k)), k * size, size)

        for turn in (0, 1):
            head, foot = left_over(rows, pieces, turn)
            for e in cut_pieces(rows, pieces):
                low, high = max(e * size, head), min((e + 1) * size, rows - foot)
                if high > low:
                    @pl.when(jnp.logical_and(k == e, here["py"] % 2 == turn))
                    def _(e=e, low=low, high=high):
                        act(sums_copy(e, pl.ds(low, high - low)), low, high - low)

    def over_pieces(act):
        def one(p, carry):
            act(piece(p))
            return carry
        lax.fori_loop(0, pieces, one, 0)

    load_copy(0, half).start()
    barrier = pltpu.get_barrier_semaphore()
    count = 0
    patient = here["py"] % 2 == 0
    for name, side in (("px", 0), ("px", 1), ("pz", 1), ("py", 0), ("py", 1)):
        there = has(name, side)
        heard = has(name, 0 if name == "pz" else side)
        if name == "py":
            there, heard = (jnp.logical_and(there, jnp.logical_not(patient)),
                            jnp.logical_and(heard, patient))
        count = count + heard.astype(jnp.int32)

        @pl.when(there)
        def _(name=name, side=side):
            pl.semaphore_signal(
                barrier, inc=1, device_id=beside(name, side), device_id_type=MESH)

    def after_first(act):
        def one(p, carry):
            act(piece(p))
            return carry
        lax.fori_loop(1, pieces, one, 0)

    def start(copy, side):
        copy(side, side).start()

    def first_x(k):
        load_copy(0, k).wait()
        each_side(0, k, start, rest=())

    pl.semaphore_wait(barrier, count)
    for side in (0, 1):
        @pl.when(has("px", side))
        def _(side=side):
            x_copy(0, side, half, side, first=True).start()
    after_first(lambda k: load_copy(0, k).start())
    load_copy(0, half).wait()
    after_first(first_x)
    load_copy(1, 0).start()
    load_copy(2, 0).start()
    over_pieces(lambda k: each_side(0, k, start, x=False, rest=(0,)))
    for side in (0, 1):
        @pl.when(jnp.logical_and(has("py", side), patient))
        def _(side=side):
            y_copy(0, side, side).start()

    @pl.when(has("pz", 1))
    def _():
        z_copy(0, 0, half, 1).wait_recv()
        over_pieces(lambda k: z_copy(0, 1, k, 1).start())

    for side in (0, 1):
        @pl.when(jnp.logical_and(has("py", side), jnp.logical_not(patient)))
        def _(side=side):
            y_copy(0, 1 - side, side).wait_recv()
            y_copy(0, side, side).start()

    for side in (0, 1):
        for slot in (0, 1):
            @pl.when(jnp.logical_not(has("py", side)))
            def _(side=side, slot=slot):
                u[slot, rows + 1 if side else 0, 1:width + 1] = jnp.zeros(
                    (width, height, lanes), jnp.float32)

            @pl.when(jnp.logical_not(has("px", side)))
            def _(side=side, slot=slot):
                def clear(r, carry):
                    u[slot, r + 1, width + 1 if side else 0] = jnp.zeros(
                        (height, lanes), jnp.float32)
                    return carry
                lax.fori_loop(0, rows, clear, 0)

            @pl.when(jnp.logical_not(has("pz", side)))
            def _(side=side, slot=slot):
                def clear(r, carry):
                    zh[slot, side, r] = jnp.zeros((width, 1, lanes), jnp.float32)
                    return carry
                lax.fori_loop(0, rows, clear, 0)

    level = lax.broadcasted_iota(jnp.int32, (width, height, lanes), 1)

    for step in range(1, STEPS + 1):
        old, new = (step - 1) % 2, step % 2

        def row(r, old, new, final):
            centre = u[old, r + 1, 1:width + 1]
            below = jnp.where(
                level == 0, zh[old, 0, r], pltpu.roll(centre, 1, axis=1))
            above = jnp.where(
                level == height - 1, zh[old, 1, r], pltpu.roll(centre, height - 1, axis=1))
            spread = (
                u[old, r, 1:width + 1]
                + u[old, r + 2, 1:width + 1]
                + u[old, r + 1, 0:width]
                + u[old, r + 1, 2:width + 2]
                + below
                + above
                - 6.0 * centre
            )
            value = centre + c[r] * spread + s[r]
            if final:
                s[r] = value
            else:
                u[new, r + 1, 1:width + 1] = value
            if final and pair:
                mean = jnp.sum(value, axis=0) * (1.0 / width)
                apart = value - mean[None]
                sq[r, 0] = mean
                sq[r, 1] = jnp.sum(apart * apart, axis=0)

        def sweep(k, step=step, old=old, new=new):
            arrived(old, k, step == 1)
            if 2 <= step < STEPS:
                sent(new, k)

            def one(i, carry):
                row(k * size + i, old, new, step == STEPS)
                return carry
            lax.fori_loop(0, size, one, 0)
            if step < STEPS:
                send(new, k)
            elif pair:
                each_sum(k, lambda copy, first, count: copy.start())

        if step == 1:
            load_copy(1, 0).wait()
            load_copy(2, 0).wait()
        over_pieces(sweep)

    def finish(copy, first, count):
        copy.wait_recv()

        def one(i, carry):
            r = first + i
            c[r] = normalise(s[r], sq[r], sqr[r])
            return carry
        lax.fori_loop(0, count, one, 0)

    def close(k):
        for slot in sorted({(STEPS - 1) % 2, (STEPS - 2) % 2}):
            sent(slot, k)
        if pair:
            each_sum(k, lambda copy, first, count: copy.wait_send())

    if pair:
        over_pieces(lambda k: each_sum(k, finish))
    over_pieces(close)


def copy_all(copies):
    for copy in copies:
        copy.start()
    for copy in copies:
        copy.wait()


def put_out(pieces, count, *refs):
    held, out, done = refs[:count], refs[count:2 * count], refs[-1]
    size = held[0].shape[0] // pieces
    copy_all([
        pltpu.make_async_copy(
            held[i].at[pl.ds(k * size, size)], out[i].at[pl.ds(k * size, size)], done.at[i, k])
        for k in range(pieces)
        for i in range(count)
    ])


def put_most(pieces, result, end, result_out, end_out, mark, done):
    rows = end.shape[0]
    size = rows // pieces
    mark[...] = jnp.zeros(mark.shape, mark.dtype)
    for turn in (0, 1):
        @pl.when(lax.axis_index("py") % 2 == turn)
        def _(turn=turn):
            head, foot = left_over(rows, pieces, turn)
            copies = []
            for k in range(pieces):
                whole = pl.ds(k * size, size)
                copies.append(pltpu.make_async_copy(
                    end.at[whole], end_out.at[whole], done.at[0, k]))
                low, high = max(k * size, head), min((k + 1) * size, rows - foot)
                if high > low:
                    part = pl.ds(low, high - low)
                    copies.append(pltpu.make_async_copy(
                        result.at[part], result_out.at[part], done.at[1, k]))
            copy_all(copies)


def left_parts(rows, pieces, turn):
    size = rows // pieces
    head, foot = left_over(rows, pieces, turn)
    parts = [(rows - foot + i, head + i, min(size, foot - i)) for i in range(0, foot, size)]
    low = head
    while low > 0:
        count = min(low, size // 2, max(low // 2, size // 8, 1))
        low -= count
        parts.append((low, low, count))
    return parts


def exchange_rest(pieces, sums, end, mark, out, other, sent, got):
    rows = end.shape[0]
    partner = {"px": 1 - lax.axis_index("px")}
    for turn in (0, 1):
        parts = left_parts(rows, pieces, turn)
        if not parts:
            continue

        @pl.when(lax.axis_index("py") % 2 == turn)
        def _(parts=parts):
            barrier = pltpu.get_barrier_semaphore()
            pl.semaphore_signal(barrier, inc=1, device_id=partner, device_id_type=MESH)
            pl.semaphore_wait(barrier, 1)
            copies = [
                pltpu.make_async_remote_copy(
                    src_ref=sums.at[pl.ds(row, count)], dst_ref=other.at[pl.ds(at, count)],
                    send_sem=sent.at[n], recv_sem=got.at[n],
                    device_id=partner, device_id_type=MESH)
                for n, (row, at, count) in enumerate(parts)
            ]
            for copy in copies:
                copy.start()
            for copy, (row, at, count) in zip(copies, parts):
                copy.wait_recv()

                def one(i, carry, row=row, at=at):
                    out[at + i] = normalise(end[row + i], sums[row + i], other[at + i])
                    return carry
                lax.fori_loop(0, count, one, 0)
            for copy in copies:
                copy.wait_send()


def put_rest(pieces, rest, result, result_out, done):
    rows = result.shape[0]
    for turn in (0, 1):
        @pl.when(lax.axis_index("py") % 2 == turn)
        def _(turn=turn):
            head, foot = left_over(rows, pieces, turn)
            pairs = [((rows - foot, head), foot), ((0, 0), head)]
            copy_all([
                pltpu.make_async_copy(
                    rest.at[pl.ds(at, count)], result_out.at[pl.ds(row, count)], done.at[n])
                for n, ((row, at), count) in enumerate(pairs) if count
            ])


def body(starting_state, scaled_conductivity, scaled_heat_supply):
    rows, width, height, lanes = starting_state.shape
    pieces = next(n for n in (8, 4, 2) if rows % n == 0)
    pair = lax.axis_size("px") == 2
    dma = pltpu.SemaphoreType.DMA
    block = jax.ShapeDtypeStruct(starting_state.shape, jnp.float32)
    field = pltpu.VMEM((rows, width, height, lanes), jnp.float32)
    sums = pltpu.VMEM((rows, 2, height, lanes), jnp.float32)
    here, there = pl.BlockSpec(memory_space=pltpu.VMEM), pl.BlockSpec(memory_space=pl.ANY)
    scratch = [
        pltpu.VMEM((2, rows + 2, width + 2, height, lanes), jnp.float32),
        pltpu.VMEM((2, 2, rows, width, 1, lanes), jnp.float32),
    ]
    scratch += [sums] if pair else [field]
    scratch += [
        dma((2, pieces)),
        dma((2, 1 if pair else 2, pieces)), dma((2, 1 if pair else 2, pieces)),
        dma((2, 2)), dma((2, 2)),
        dma((2, 2, pieces)), dma((2, 2, pieces)),
    ]
    scratch += [dma((pieces,)), dma((pieces,))] if pair else []
    made = (field, field, sums) if pair else (field,)
    outputs = pl.pallas_call(
        functools.partial(kernel, pieces, pair),
        out_shape=made,
        in_specs=[there] * 3,
        out_specs=(here,) * len(made),
        scratch_shapes=scratch,
        compiler_params=pltpu.CompilerParams(
            collective_id=0, has_side_effects=True, vmem_limit_bytes=(34 if pair else 40) * 1024 * 1024),
    )(starting_state, scaled_conductivity, scaled_heat_supply)
    if pair:
        held, end, kept = outputs
        result, end_out, mark = pl.pallas_call(
            functools.partial(put_most, pieces),
            out_shape=(block, block, pltpu.VMEM((8, 128), jnp.float32)),
            in_specs=[here] * 2,
            out_specs=(there, there, here),
            scratch_shapes=[dma((2, pieces))],
            compiler_params=pltpu.CompilerParams(vmem_limit_bytes=1024 * 1024),
        )(held, end)
        most = max(sum(left_over(rows, pieces, turn)) for turn in (0, 1))
        parts = max(len(left_parts(rows, pieces, turn)) for turn in (0, 1))
        rest = pl.pallas_call(
            functools.partial(exchange_rest, pieces),
            out_shape=pltpu.VMEM((most, width, height, lanes), jnp.float32),
            in_specs=[here] * 3,
            out_specs=here,
            scratch_shapes=[
                pltpu.VMEM((most, 2, height, lanes), jnp.float32), dma((parts,)), dma((parts,))],
            compiler_params=pltpu.CompilerParams(
                collective_id=1, has_side_effects=True, vmem_limit_bytes=4 * 1024 * 1024),
        )(kept, end, mark)
        result = pl.pallas_call(
            functools.partial(put_rest, pieces),
            out_shape=block,
            in_specs=[here, there],
            out_specs=there,
            scratch_shapes=[dma((2,))],
            input_output_aliases={1: 0},
            compiler_params=pltpu.CompilerParams(vmem_limit_bytes=1024 * 1024),
        )(rest, result)
        return result, end_out
    outputs = pl.pallas_call(
        functools.partial(put_out, pieces, len(outputs)),
        out_shape=(block,) * len(outputs),
        in_specs=[here] * len(outputs),
        out_specs=(there,) * len(outputs),
        scratch_shapes=[dma((len(outputs), pieces))],
        compiler_params=pltpu.CompilerParams(vmem_limit_bytes=1024 * 1024),
    )(*outputs)
    (end,) = outputs
    line = width * lax.axis_size("px")
    guess = 1.0
    moved = end - guess
    totals, squares = lax.psum(
        (jnp.sum(moved, axis=1, keepdims=True), jnp.sum(moved * moved, axis=1, keepdims=True)), "px"
    )
    row_average = guess + totals / line
    line_variance = squares / line - totals / line * (totals / line)
    return ((end - row_average) * lax.rsqrt(line_variance + 0.0001), end)


def solution(mesh):
    placed = P("py", "px", "pz", None)
    return jax.shard_map(
        body,
        mesh=mesh,
        in_specs=(placed, placed, placed),
        out_specs=(placed, placed),
        check_vma=False,
    )
```
